32 devices in a mesh: groups: 2 (over y), axial: 16 (over z, x, core).
Axes of the slice: x: 2, y: 2, z: 4, core: 2. Of those that a mesh axis runs over, the one named last changes fastest.
Arguments:
- pair_rep: bfloat16 [192, 96, 128], P(('groups', 'axial')), parts along dimension 0, may hold values from -6 to 6
- norm_out: float32 [128], replicated, may hold values from 0.5 to 1.5
- proj_out: bfloat16 [128, 512], replicated, may hold values from -0.5 to 0.5
- gate_out: bfloat16 [128, 128], replicated, may hold values from -0.5 to 0.5
- mid_out: float32 [128], replicated, may hold values from 0.5 to 1.5
- final_out: bfloat16 [128, 128], replicated, may hold values from -0.5 to 0.5
- norm_in: float32 [128], replicated, may hold values from 0.5 to 1.5
- proj_in: bfloat16 [128, 512], replicated, may hold values from -0.5 to 0.5
- gate_in: bfloat16 [128, 128], replicated, may hold values from -0.5 to 0.5
- mid_in: float32 [128], replicated, may hold values from 0.5 to 1.5
- final_in: bfloat16 [128, 128], replicated, may hold values from -0.5 to 0.5
Outputs:
- updated: bfloat16 [192, 96, 128], P(('groups', 'axial')), parts along dimension 0
The draws below stay inside these ranges and needn't reach their ends.
There are 2 independent parts, one for each index of `groups`. The reference program is written for one: setup_inputs(seed, part) draws one part's arguments, and reference() takes and returns one part's arrays. A program takes and returns all parts, laid end to end along the dimension named above; an argument that names none is the same for every part. Nothing has to cross between parts.
All inputs are finite; a program needn't handle non-finite values.
Results may differ from the reference program's by a relative error of at most 0.013.
Values may be sent and summed in bfloat16 or wider, within the bound.
A program may use at most 64 MiB of HBM per device.

```python
import math
import jax
import jax.numpy as jnp
from jax import lax

C = 128
HID = 128
N = 96


def levels(rng, shape, cuts, smallest, high):
    loudness = 1.0
    for dim, parts in cuts:
        heights = jax.random.uniform(jax.random.fold_in(jax.random.fold_in(rng, 6), dim), (parts,), jnp.float32, smallest / len(cuts), high / len(cuts))
        loudness = loudness * jnp.repeat(jnp.exp(heights), shape[dim] // parts).reshape((-1,) + (1,) * (len(shape) - 1 - dim))
    return loudness


def bell_draw(stream_key, shape, width, limit, shards=(), kind=jnp.bfloat16):
    drawn = jax.random.normal(stream_key, shape, jnp.float32) * width
    if len(shards) > 0:
        drawn = levels(stream_key, shape, shards, -0.22, 0.18) * drawn
    return jnp.clip(drawn, min=-limit, max=limit).astype(kind)


def setup_inputs(seed: int = 0, part: int = 0) -> dict:
    seeds = jax.random.split(jax.random.key(seed), 12)
    part_keys = jax.random.split(jax.random.fold_in(seeds[11], part), 12)
    pair_rep = bell_draw(part_keys[0], (N, N, C), 1.0, 6.0, ((0, 16),))
    norm_out = jnp.clip(1.0 + 0.1 * jax.random.normal(seeds[1], (C,), jnp.float32), 0.5, 1.5)
    proj_out = bell_draw(seeds[2], (C, 4 * HID), C ** -0.5, 0.5)
    gate_out = bell_draw(seeds[3], (C, C), C ** -0.5, 0.5)
    mid_out = jnp.clip(1.0 + 0.1 * jax.random.normal(seeds[4], (HID,), jnp.float32), 0.5, 1.5)
    final_out = bell_draw(seeds[5], (HID, C), HID ** -0.5, 0.5)
    norm_in = jnp.clip(1.0 + 0.1 * jax.random.normal(seeds[6], (C,), jnp.float32), 0.5, 1.5)
    proj_in = bell_draw(seeds[7], (C, 4 * HID), C ** -0.5, 0.5)
    gate_in = bell_draw(seeds[8], (C, C), C ** -0.5, 0.5)
    mid_in = jnp.clip(1.0 + 0.1 * jax.random.normal(seeds[9], (HID,), jnp.float32), 0.5, 1.5)
    final_in = bell_draw(seeds[10], (HID, C), HID ** -0.5, 0.5)
    return {"pair_rep": pair_rep, "norm_out": norm_out, "proj_out": proj_out, "gate_out": gate_out, "mid_out": mid_out, "final_out": final_out, "norm_in": norm_in, "proj_in": proj_in, "gate_in": gate_in, "mid_in": mid_in, "final_in": final_in}


EPS = 1e-05

def normalize(values, gain, axis):
    average = lax.optimization_barrier(jnp.mean(values, axis=axis, keepdims=True))
    spread = lax.optimization_barrier(jnp.mean(jnp.square(values - average), axis=axis, keepdims=True))
    return (values - average) * lax.rsqrt(spread + EPS) * gain

def project_rows(rows_in, norm_gain, weights):
    normed = normalize(rows_in.astype(jnp.float32), norm_gain, -1).astype(jnp.bfloat16)
    projected = jnp.einsum('rnc,ck->krn', normed.astype(jnp.float32), weights.astype(jnp.float32))
    hidden = weights.shape[1] // 4
    left_side = (jax.nn.sigmoid(projected[hidden:2 * hidden]) * projected[:hidden]).astype(jnp.bfloat16)
    right_side = (jax.nn.sigmoid(projected[3 * hidden:]) * projected[2 * hidden:3 * hidden]).astype(jnp.bfloat16)
    return (left_side, right_side, normed)

def triangle(left_side, right_side, outgoing):
    hidden = left_side.shape[0]
    extent = left_side.shape[1]
    group_size = math.gcd(hidden, 16)
    left_groups = left_side.reshape(hidden // group_size, group_size, extent, extent)
    right_groups = right_side.reshape(hidden // group_size, group_size, extent, extent)
    formula = 'kil,kjl->kij' if outgoing else 'kli,klj->kij'

    def one_group(operands):
        return jnp.einsum(formula, operands[0].astype(jnp.float32), operands[1].astype(jnp.float32)).astype(jnp.bfloat16)
    return lax.map(one_group, (left_groups, right_groups)).reshape(hidden, extent, extent)

def update(pair_rep, norm_gain, weights, gate_weight, mid_gain, final_weight, outgoing):
    extent = pair_rep.shape[0]
    channels = pair_rep.shape[2]
    hidden = weights.shape[1] // 4
    block_rows = math.gcd(extent, 64)
    block_count = extent // block_rows
    blocks = pair_rep.reshape(block_count, block_rows, extent, channels)
    left_side, right_side, normed = lax.map(lambda rows_in: project_rows(rows_in, norm_gain, weights), blocks)
    left_side = jnp.transpose(left_side, (1, 0, 2, 3)).reshape(hidden, extent, extent)
    right_side = jnp.transpose(right_side, (1, 0, 2, 3)).reshape(hidden, extent, extent)
    tri = triangle(left_side, right_side, outgoing)
    tri_blocks = jnp.transpose(tri.reshape(hidden, block_count, block_rows, extent), (1, 0, 2, 3))

    def finish(operands):
        rows_in, normed_rows, tri_rows = operands
        gating = jax.nn.sigmoid(jnp.einsum('rnc,ce->rne', normed_rows.astype(jnp.float32), gate_weight.astype(jnp.float32)))
        tri_normed = normalize(tri_rows.astype(jnp.float32), mid_gain[:, None, None], 0).astype(jnp.bfloat16)
        result = jnp.einsum('krn,kc->rnc', tri_normed.astype(jnp.float32), final_weight.astype(jnp.float32))
        return (rows_in.astype(jnp.float32) + gating * result).astype(jnp.bfloat16)
    return lax.map(finish, (blocks, normed, tri_blocks)).reshape(extent, extent, channels)

def reference(pair_rep, norm_out, proj_out, gate_out, mid_out, final_out, norm_in, proj_in, gate_in, mid_in, final_in):
    first = update(pair_rep, norm_out, proj_out, gate_out, mid_out, final_out, True)
    return update(first, norm_in, proj_in, gate_in, mid_in, final_in, False)
```

```python
import functools

import jax
import jax.numpy as jnp
from jax import lax
from jax.experimental import pallas as pl
from jax.experimental.pallas import tpu as pltpu
from jax.sharding import PartitionSpec as P

EPS = 1e-05


def normalize(values, gain, axis):
    average = jnp.mean(values, axis=axis, keepdims=True)
    spread = jnp.mean(jnp.square(values - average), axis=axis, keepdims=True)
    return (values - average) * lax.rsqrt(spread + EPS) * gain


def channel_product(left_side, right_side, outgoing):
    formula = "kil,kjl->kij" if outgoing else "kli,klj->kij"
    got_left, got_right = (
        lax.all_to_all(left_side, "axial", split_axis=0, concat_axis=1, tiled=True),
        lax.all_to_all(right_side, "axial", split_axis=0, concat_axis=1, tiled=True),
    )
    return jnp.einsum(formula, got_left, got_right, preferred_element_type=jnp.float32)


def update(pair_rep, norm_gain, weights, gate_weight, mid_gain, final_weight, outgoing):
    normed = normalize(pair_rep.astype(jnp.float32), norm_gain, -1).astype(jnp.bfloat16)
    projected = jnp.einsum("rnc,ck->krn", normed, weights, preferred_element_type=jnp.float32)
    hidden = weights.shape[1] // 4
    left_side = (jax.nn.sigmoid(projected[hidden : 2 * hidden]) * projected[:hidden]).astype(
        jnp.bfloat16
    )
    right_side = (
        jax.nn.sigmoid(projected[3 * hidden :]) * projected[2 * hidden : 3 * hidden]
    ).astype(jnp.bfloat16)
    product = channel_product(left_side, right_side, outgoing)
    tri = lax.all_to_all(
        product.astype(jnp.bfloat16), "axial", split_axis=1, concat_axis=0, tiled=True
    )
    gating = jax.nn.sigmoid(
        jnp.einsum("rnc,ce->rne", normed, gate_weight, preferred_element_type=jnp.float32)
    )
    tri_normed = normalize(tri.astype(jnp.float32), mid_gain[:, None, None], 0).astype(jnp.bfloat16)
    result = jnp.einsum("krn,kc->rnc", tri_normed, final_weight, preferred_element_type=jnp.float32)
    return (pair_rep.astype(jnp.float32) + gating * result).astype(jnp.bfloat16)


MESH = pl.DeviceIdType.MESH
CORES = 2
SIDES = 2
QUAD = CORES * SIDES
UP, DOWN = range(2)
OWN, PEER, ACROSS, CORNER = range(4)
NEAR, FAR, ALL = (OWN, PEER), (ACROSS, CORNER), (OWN, PEER, ACROSS, CORNER)
SUB = 8
LINE = 4
PIECES = 3
VMEM_BYTES = 56 * 1024 * 1024


def fits(devices, pair_shape, proj_shape):
    rows, tokens, channels = pair_shape
    hidden = proj_shape[1] // 4
    block = rows * tokens * hidden * 4
    return (
        devices == QUAD * LINE
        and devices * rows == tokens
        and rows <= SUB
        and rows % PIECES == 0
        and tokens % 16 == 0
        and channels == hidden
        and hidden % 128 == 0
        and (4 * (devices // QUAD) + 24) * block < VMEM_BYTES // 2
    )


def layer_norm(values, gain):
    average = jnp.mean(values, axis=-1, keepdims=True)
    centred = values - average
    spread = jnp.mean(jnp.square(centred), axis=-1, keepdims=True)
    return centred * lax.rsqrt(spread + EPS) * gain


def dot(left, right):
    return jnp.dot(left, right, preferred_element_type=jnp.float32)


def line_kernel(
    devices,
    pieces,
    pair_ref,
    norm_out,
    proj_out,
    gate_out,
    mid_out,
    final_out,
    norm_in,
    proj_in,
    gate_in,
    mid_in,
    final_in,
    out_ref,
    held,
    fixed,
    fixed_f32,
    moving,
    normed_ref,
    raw_ref,
    resid,
    gating,
    tri,
    closed,
    landed,
    turned,
    line_send,
    line_recv,
    fixed_send,
    fixed_recv,
    closed_send,
    closed_recv,
):
    rows, tokens, channels = pair_ref.shape
    hidden = fixed.shape[-1]
    length = devices // QUAD
    piece = rows // pieces
    me = lax.axis_index("axial")
    core = me % CORES
    side = (me // CORES) % SIDES
    line = me // QUAD
    seats = (
        side * CORES + core,
        side * CORES + 1 - core,
        (1 - side) * CORES + core,
        (1 - side) * CORES + 1 - core,
    )
    seat = seats[OWN]

    def mate(which):
        return line * QUAD + seats[which]

    targets = {
        UP: jnp.minimum(line + 1, length - 1) * QUAD + seat,
        DOWN: jnp.maximum(line - 1, 0) * QUAD + seat,
    }

    inner = jnp.logical_and(line > 0, line < length - 1)
    onward = jnp.where(2 * line < length, 1, -1)
    first_block = line + onward
    second_block = jnp.where(inner, line - onward, line)
    third_block = line + 2 * onward
    fourth_block = jnp.where(inner, line, line + 3 * onward)

    def remote(source, target, sent, got, device):
        return pltpu.make_async_remote_copy(
            src_ref=source,
            dst_ref=target,
            send_sem=sent,
            recv_sem=got,
            device_id={"axial": device},
            device_id_type=MESH,
        )

    def window(part):
        return pl.ds(part * piece, piece)

    def line_copy(phase, way, block, part, source=None):
        there = held.at[phase, block, window(part)]
        return remote(
            there if source is None else source.at[window(part)],
            there,
            line_send.at[phase, way, block, part],
            line_recv.at[phase, block, part],
            targets[way],
        )

    def pass_on(phase, block, part, act, source=None):
        @pl.when(jnp.logical_and(block <= line, line < length - 1))
        def _():
            act(line_copy(phase, UP, block, part, source))

        @pl.when(jnp.logical_and(block >= line, line > 0))
        def _():
            act(line_copy(phase, DOWN, block, part, source))

    def start(descriptor):
        descriptor.start()

    def finish_send(descriptor):
        descriptor.wait_send()

    def fixed_copy(phase, which, to):
        there = fixed.at[phase, seats[which]]
        return remote(
            there,
            there,
            fixed_send.at[phase, which, to],
            fixed_recv.at[phase, seats[which]],
            mate(to),
        )

    def closed_copy(phase, block, which, span):
        return remote(
            closed.at[phase, block, which, span],
            landed.at[phase, block, seat, span],
            closed_send.at[phase, block, which],
            closed_recv.at[phase, block, seat],
            mate(which),
        )

    def closed_wait(phase, block, which):
        remote(
            closed.at[phase, block, which],
            landed.at[phase, block, seats[which]],
            closed_send.at[phase, block, which],
            closed_recv.at[phase, block, seats[which]],
            mate(which),
        ).wait_recv()

    def flat(values):
        return values.reshape(-1, values.shape[-1])

    def gated(projected):
        return (jax.nn.sigmoid(projected[:, hidden:]) * projected[:, :hidden]).astype(jnp.bfloat16)

    def own_side(phase, block, norm, weights):
        normed = layer_norm(flat(block).astype(jnp.float32), norm[...]).astype(jnp.bfloat16)
        made = gated(dot(normed, weights)).reshape(rows, tokens, hidden)
        fixed[phase, seat] = made
        fixed_f32[OWN] = made.astype(jnp.float32)

    def take_fixed(phase, which):
        fixed_copy(phase, which, PEER).wait_recv()
        fixed_f32[which] = fixed[phase, seats[which]].astype(jnp.float32)

    def prepare(phase, block, first, count, norm, weights, gate):
        span = pl.ds(first, count)
        raw = held[phase, block, span].astype(jnp.float32)
        normed = layer_norm(flat(raw), norm[...])
        raw_ref[:count, :tokens] = raw
        normed_ref[:count, :tokens] = normed.reshape(count, tokens, channels)
        made = gated(dot(normed.astype(jnp.bfloat16), weights))
        moving[block, span] = made.astype(jnp.float32).reshape(count, tokens, hidden)
        picked = []
        for row in range(count):
            for which in range(QUAD):
                at = pl.ds(line * (QUAD * rows) + seats[which] * rows, SUB)
                picked.append(normed_ref[row, at, :])
                resid[block, first + row, which] = raw_ref[row, at, :]
        picked = jnp.concatenate(picked, axis=0).astype(jnp.bfloat16)
        opened = jax.nn.sigmoid(dot(picked, gate[...]))
        gating[block, span] = opened.reshape(count, QUAD, SUB, channels)

    def multiply(phase, block, first, count, group, mid, final):
        def one(row, carry):
            right = moving[block, first + row]
            for which in group:
                total = jnp.sum(fixed_f32[which] * right[None], axis=1)
                tri[row, which, :rows, :] = total
            return carry

        lax.fori_loop(0, count, one, 0)
        lanes = slice(group[0], group[0] + len(group))
        product = flat(tri[:count, lanes]).astype(jnp.bfloat16).astype(jnp.float32)
        normed = layer_norm(product, mid[...]).astype(jnp.bfloat16)
        result = dot(normed, final[...]).reshape(count, len(group), SUB, channels)
        span = pl.ds(first, count)
        result = resid[block, span, lanes] + gating[block, span, lanes] * result
        result = result.astype(jnp.bfloat16)
        for place, which in enumerate(group):
            if which == OWN:
                landed[phase, block, seat, span] = result[:, place]
            else:
                closed[phase, block, which, span] = result[:, place]
        for which in group:
            if which != OWN:
                closed_copy(phase, block, which, span).start()

    def exchange(phase, norm, weights, gate, mid, final):
        def ready(block, first=0, count=rows):
            prepare(phase, block, first, count, norm, weights, gate)

        def join(block, group, first=0, count=rows):
            multiply(phase, block, first, count, group, mid, final)

        def arrive(block, part):
            line_copy(phase, UP, block, part).wait_recv()
            pass_on(phase, block, part, start)

        def slot(at):
            step, part = at // pieces, at % pieces
            if step == 0:
                arrive(first_block, part)

                @pl.when(inner)
                def _():
                    arrive(second_block, part)
            elif step == 1:
                arrive(third_block, part)
            else:

                @pl.when(jnp.logical_not(inner))
                def _():
                    arrive(fourth_block, part)

        ready(line)
        take_fixed(phase, PEER)
        join(line, NEAR)
        for at in range(pieces):
            slot(at)
        take_fixed(phase, ACROSS)
        fixed_copy(phase, ACROSS, PEER).start()
        ready(first_block)
        take_fixed(phase, CORNER)
        join(line, FAR)
        slot(pieces)
        join(first_block, ALL)
        slot(pieces + 1)

        @pl.when(inner)
        def _():
            ready(second_block)
            join(second_block, ALL)

        slot(pieces + 2)
        ready(third_block)
        join(third_block, ALL)
        for at in range(2 * pieces, 3 * pieces):
            slot(at)
            if at % pieces:

                @pl.when(jnp.logical_not(inner))
                def _():
                    begin = 0 if at % pieces == 1 else 2 * piece
                    count = 2 * piece if begin == 0 else piece
                    ready(fourth_block, begin, count)
                    join(fourth_block, ALL, begin, count)
        for block in range(length):
            for which in (PEER, ACROSS, CORNER):
                closed_wait(phase, block, which)

    def turn(phase, target, lead):
        turned[...] = landed[phase].reshape(tokens * SUB, channels).astype(jnp.float32)
        for row in range(rows):
            target[lead + (row,)] = turned[pl.ds(row, tokens, stride=SUB), :].astype(jnp.bfloat16)

    def finish(phase, source):
        for block in range(length):
            for part in range(pieces):
                pass_on(phase, block, part, finish_send)
            for which in (PEER, ACROSS, CORNER):
                closed_copy(phase, block, which, pl.ds(0, rows)).wait_send()
        fixed_copy(phase, OWN, PEER).wait_send()
        fixed_copy(phase, OWN, ACROSS).wait_send()
        fixed_copy(phase, ACROSS, PEER).wait_send()

    barrier = pltpu.get_barrier_semaphore()

    def greet(device):
        pl.semaphore_signal(barrier, inc=1, device_id={"axial": device}, device_id_type=MESH)

    for which in (PEER, ACROSS, CORNER):
        greet(mate(which))

    @pl.when(line < length - 1)
    def _():
        greet(targets[UP])

    @pl.when(line > 0)
    def _():
        greet(targets[DOWN])

    held[0, line] = pair_ref[...]
    tri[...] = jnp.zeros_like(tri)
    normed_ref[...] = jnp.zeros_like(normed_ref)
    raw_ref[...] = jnp.zeros_like(raw_ref)
    half = 2 * hidden
    own_side(0, pair_ref[...], norm_out, proj_out[:, half:])
    ends = (line > 0).astype(jnp.int32) + (line < length - 1).astype(jnp.int32)
    pl.semaphore_wait(barrier, QUAD - 1 + ends)
    for part in range(pieces):
        pass_on(0, line, part, start, pair_ref)
    fixed_copy(0, OWN, ACROSS).start()
    fixed_copy(0, OWN, PEER).start()
    exchange(0, norm_out, proj_out[:, :half], gate_out, mid_out, final_out)
    turn(0, held, (1, line))
    for part in range(pieces):
        pass_on(1, line, part, start)
    own_side(1, held[1, line], norm_in, proj_in[:, :half])
    fixed_copy(1, OWN, ACROSS).start()
    fixed_copy(1, OWN, PEER).start()
    exchange(1, norm_in, proj_in[:, half:], gate_in, mid_in, final_in)
    turn(1, out_ref, ())
    finish(0, pair_ref)
    finish(1, held)


def gather_rows(devices, pair_rep, *weights):
    rows, tokens, channels = pair_rep.shape
    hidden = weights[1].shape[1] // 4
    gains = [w.reshape(1, -1) if w.ndim == 1 else w for w in weights]
    length = devices // QUAD
    pieces = PIECES
    block = (rows, tokens, hidden)
    low, full = jnp.bfloat16, jnp.float32
    spot = (QUAD, rows, SUB, channels)
    return pl.pallas_call(
        functools.partial(line_kernel, devices, pieces),
        out_shape=jax.ShapeDtypeStruct(pair_rep.shape, pair_rep.dtype),
        in_specs=[pl.BlockSpec(memory_space=pltpu.VMEM)] * 11,
        out_specs=pl.BlockSpec(memory_space=pltpu.VMEM),
        scratch_shapes=[
            pltpu.VMEM((2, length) + block, low),
            pltpu.VMEM((2, QUAD) + block, low),
            pltpu.VMEM((QUAD,) + block, full),
            pltpu.VMEM((length,) + block, full),
            pltpu.VMEM((rows, tokens + SUB, channels), full),
            pltpu.VMEM((rows, tokens + SUB, channels), full),
            pltpu.VMEM((length, rows, QUAD, SUB, channels), full),
            pltpu.VMEM((length, rows, QUAD, SUB, channels), full),
            pltpu.VMEM((rows, QUAD, SUB, channels), full),
            pltpu.VMEM((2, length) + spot, low),
            pltpu.VMEM((2, length) + spot, low),
            pltpu.VMEM((tokens * SUB, channels), full),
            pltpu.SemaphoreType.DMA((2, 2, length, pieces)),
            pltpu.SemaphoreType.DMA((2, length, pieces)),
            pltpu.SemaphoreType.DMA((2, QUAD, QUAD)),
            pltpu.SemaphoreType.DMA((2, QUAD)),
            pltpu.SemaphoreType.DMA((2, length, QUAD)),
            pltpu.SemaphoreType.DMA((2, length, QUAD)),
        ],
        compiler_params=pltpu.CompilerParams(
            collective_id=0, has_side_effects=True, vmem_limit_bytes=VMEM_BYTES
        ),
        name="gather_rows",
    )(pair_rep, *gains)


def exchange_channels(
    pair_rep,
    norm_out,
    proj_out,
    gate_out,
    mid_out,
    final_out,
    norm_in,
    proj_in,
    gate_in,
    mid_in,
    final_in,
):
    first = update(pair_rep, norm_out, proj_out, gate_out, mid_out, final_out, True)
    return update(first, norm_in, proj_in, gate_in, mid_in, final_in, False)


def solution(mesh):
    devices = mesh.shape["axial"]

    def on_device(*arrays):
        if fits(devices, arrays[0].shape, arrays[2].shape):
            return gather_rows(devices, *arrays)
        return exchange_channels(*arrays)

    placed = (P(("groups", "axial"), None, None), P(), P(), P(), P(), P(), P(), P(), P(), P(), P())
    return jax.shard_map(
        on_device,
        mesh=mesh,
        in_specs=placed,
        out_specs=P(("groups", "axial"), None, None),
        check_vma=False,
    )
```

```python
import functools

import jax
import jax.numpy as jnp
from jax import lax
from jax.experimental import pallas as pl
from jax.experimental.pallas import tpu as pltpu
from jax.sharding import PartitionSpec as P

EPS = 1e-05


def normalize(values, gain, axis):
    average = jnp.mean(values, axis=axis, keepdims=True)
    spread = jnp.mean(jnp.square(values - average), axis=axis, keepdims=True)
    return (values - average) * lax.rsqrt(spread + EPS) * gain


def channel_product(left_side, right_side, outgoing):
    formula = "kil,kjl->kij" if outgoing else "kli,klj->kij"
    got_left, got_right = (
        lax.all_to_all(left_side, "axial", split_axis=0, concat_axis=1, tiled=True),
        lax.all_to_all(right_side, "axial", split_axis=0, concat_axis=1, tiled=True),
    )
    return jnp.einsum(formula, got_left, got_right, preferred_element_type=jnp.float32)


def update(pair_rep, norm_gain, weights, gate_weight, mid_gain, final_weight, outgoing):
    normed = normalize(pair_rep.astype(jnp.float32), norm_gain, -1).astype(jnp.bfloat16)
    projected = jnp.einsum("rnc,ck->krn", normed, weights, preferred_element_type=jnp.float32)
    hidden = weights.shape[1] // 4
    left_side = (jax.nn.sigmoid(projected[hidden : 2 * hidden]) * projected[:hidden]).astype(
        jnp.bfloat16
    )
    right_side = (
        jax.nn.sigmoid(projected[3 * hidden :]) * projected[2 * hidden : 3 * hidden]
    ).astype(jnp.bfloat16)
    product = channel_product(left_side, right_side, outgoing)
    tri = lax.all_to_all(
        product.astype(jnp.bfloat16), "axial", split_axis=1, concat_axis=0, tiled=True
    )
    gating = jax.nn.sigmoid(
        jnp.einsum("rnc,ce->rne", normed, gate_weight, preferred_element_type=jnp.float32)
    )
    tri_normed = normalize(tri.astype(jnp.float32), mid_gain[:, None, None], 0).astype(jnp.bfloat16)
    result = jnp.einsum("krn,kc->rnc", tri_normed, final_weight, preferred_element_type=jnp.float32)
    return (pair_rep.astype(jnp.float32) + gating * result).astype(jnp.bfloat16)


MESH = pl.DeviceIdType.MESH
CORES = 2
SIDES = 2
QUAD = CORES * 2
SAME, SIDE, OVER, BOTH = range(4)
OWN, PEER, ACROSS, CORNER = range(4)
NEAR, FAR, ALL = (OWN, PEER), (ACROSS, CORNER), (OWN, PEER, ACROSS, CORNER)
SUB = 8
HALVES = 2
INPUTS = 11
PIECES = 6
VMEM_BYTES = 56 * 1024 * 1024


def fits(devices, pair_shape, proj_shape):
    rows, tokens, channels = pair_shape
    hidden = proj_shape[1] // 4
    block = rows * tokens * hidden * 4
    return (
        devices == QUAD * SIDES * HALVES
        and devices * rows == tokens
        and rows <= SUB
        and rows % PIECES == 0
        and tokens % 16 == 0
        and channels == hidden
        and hidden % 128 == 0
        and (6 * (devices // QUAD) + 24) * block < VMEM_BYTES // 2
    )


def layer_norm(values, gain):
    average = jnp.mean(values, axis=-1, keepdims=True)
    centred = values - average
    spread = jnp.mean(jnp.square(centred), axis=-1, keepdims=True)
    return centred * lax.rsqrt(spread + EPS) * gain


def dot(left, right):
    return jnp.dot(left, right, preferred_element_type=jnp.float32)


def line_kernel(
    devices,
    pieces,
    *refs,
):
    inputs, out_ref, scratch = refs[:INPUTS], refs[INPUTS], refs[INPUTS + 1 :]
    copies, scratch = scratch[:INPUTS], scratch[INPUTS:]
    (
        pair_ref,
        norm_out,
        proj_out,
        gate_out,
        mid_out,
        final_out,
        norm_in,
        proj_in,
        gate_in,
        mid_in,
        final_in,
    ) = copies
    (
    loaded,
    held,
    fixed,
    fixed_f32,
    moving,
    normed_ref,
    raw_ref,
    resid,
    gating,
    tri,
    closed,
    landed,
    turned,
    line_send,
    line_recv,
    fixed_send,
    fixed_recv,
    closed_send,
    closed_recv,
    ) = scratch
    rows, tokens, channels = pair_ref.shape
    hidden = fixed.shape[-1]
    blocks = devices // QUAD
    piece = rows // pieces
    me = lax.axis_index("axial")
    core = me % CORES
    side = (me // CORES) % SIDES
    level = me // (CORES * SIDES)
    half, floor = level // 2, level % 2
    end = jnp.logical_or(level == 0, level == 2 * HALVES - 1)
    places = ((0, 0), (0, 1), (1, 0), (1, 1))
    seats = ((0, 0), (0, 1), (1, 1), (1, 0))

    def turned_to(value, flip):
        return 1 - value if flip else value

    def device(block, which):
        over, aside = places[block]
        up, swap = seats[which]
        at = 2 * turned_to(half, over) + turned_to(floor, up)
        return (at * SIDES + turned_to(side, aside)) * CORES + turned_to(core, swap != aside)

    def mate(which):
        return device(SAME, which)

    def remote(source, target, sent, got, device):
        return pltpu.make_async_remote_copy(
            src_ref=source,
            dst_ref=target,
            send_sem=sent,
            recv_sem=got,
            device_id={"axial": device},
            device_id_type=MESH,
        )

    def window(part):
        return pl.ds(part * piece, piece)

    def line_copy(phase, target, part, source=None):
        came = held.at[phase, OVER, window(part)]
        goes = came if target == BOTH else source.at[window(part)]
        return remote(
            goes,
            held.at[phase, target, window(part)],
            line_send.at[phase, target, part],
            line_recv.at[phase, target, part],
            device(OVER if target == OVER else SIDE, OWN),
        )

    def fixed_copy(phase, which, to):
        arrives = {(OWN, PEER): PEER, (OWN, ACROSS): ACROSS, (ACROSS, PEER): CORNER}[which, to]
        return remote(
            fixed.at[phase, which],
            fixed.at[phase, arrives],
            fixed_send.at[phase, arrives],
            fixed_recv.at[phase, arrives],
            mate(to),
        )

    def closed_copy(phase, block, which, span):
        here = device(block, OWN)
        return remote(
            closed.at[phase, block, which, span],
            landed.at[phase, here, span],
            closed_send.at[phase, block, which],
            closed_recv.at[phase, here],
            mate(which),
        )

    def closed_wait(phase, block, which):
        there = device(block, which)
        remote(
            closed.at[phase, block, which],
            landed.at[phase, there],
            closed_send.at[phase, block, which],
            closed_recv.at[phase, there],
            mate(which),
        ).wait_recv()

    def flat(values):
        return values.reshape(-1, values.shape[-1])

    def gated(projected):
        return (jax.nn.sigmoid(projected[:, hidden:]) * projected[:, :hidden]).astype(jnp.bfloat16)

    def own_side(phase, block, norm, weights):
        normed = layer_norm(flat(block).astype(jnp.float32), norm[...]).astype(jnp.bfloat16)
        made = gated(dot(normed, weights)).reshape(rows, tokens, hidden)
        fixed[phase, OWN] = made
        fixed_f32[OWN] = made.astype(jnp.float32)

    def take_fixed(phase, which):
        source = ACROSS if which == CORNER else OWN
        fixed_copy(phase, source, ACROSS if which == ACROSS else PEER).wait_recv()
        fixed_f32[which] = fixed[phase, which].astype(jnp.float32)

    def prepare(phase, source, block, first, count, norm, weights, gate):
        span = pl.ds(first, count)
        raw = source[span].astype(jnp.float32)
        normed = layer_norm(flat(raw), norm[...])
        raw_ref[:count, :tokens] = raw
        normed_ref[:count, :tokens] = normed.reshape(count, tokens, channels)
        made = gated(dot(normed.astype(jnp.bfloat16), weights))
        moving[block, span] = made.astype(jnp.float32).reshape(count, tokens, hidden)
        picked = []
        for row in range(count):
            for which in range(QUAD):
                at = pl.ds(mate(which) * rows, SUB)
                picked.append(normed_ref[row, at, :])
                resid[block, first + row, which] = raw_ref[row, at, :]
        picked = jnp.concatenate(picked, axis=0).astype(jnp.bfloat16)
        opened = jax.nn.sigmoid(dot(picked, gate[...]))
        gating[block, span] = opened.reshape(count, QUAD, SUB, channels)

    def multiply(block, first, count, group):
        def one(row, carry):
            right = moving[block, first + row]
            for which in group:
                total = jnp.sum(fixed_f32[which] * right[None], axis=1)
                tri[block, first + row, which, :rows, :] = total
            return carry

        lax.fori_loop(0, count, one, 0)

    def close(phase, jobs, mid, final):
        for job in jobs:
            multiply(*job)

        def gather(ref):
            picked = []
            for block, first, count, group in jobs:
                lanes = slice(group[0], group[-1] + 1)
                picked.append(flat(ref[block, first : first + count, lanes]))
            return jnp.concatenate(picked, axis=0) if len(picked) > 1 else picked[0]

        product = gather(tri).astype(jnp.bfloat16).astype(jnp.float32)
        normed = layer_norm(product, mid[...]).astype(jnp.bfloat16)
        result = gather(resid) + gather(gating) * dot(normed, final[...])
        result = result.astype(jnp.bfloat16)
        at = 0
        for block, first, count, group in jobs:
            size = count * len(group) * SUB
            part = result[at : at + size].reshape(count, len(group), SUB, channels)
            at += size
            span = pl.ds(first, count)
            for place, which in enumerate(group):
                if which == OWN:
                    landed[phase, device(block, OWN), span] = part[:, place]
                else:
                    closed[phase, block, which, span] = part[:, place]
        for block, first, count, group in jobs:
            for which in group:
                if which != OWN:
                    closed_copy(phase, block, which, pl.ds(first, count)).start()

    def exchange(phase, own, norm, weights, gate, mid, final):
        def ready(block, first=0, count=rows):
            source = own if block == SAME else held.at[phase, block]
            prepare(phase, source, block, first, count, norm, weights, gate)

        def join(*jobs):
            close(phase, [(block, 0, rows, group) for block, group in jobs], mid, final)

        def await_line(target, part):
            line_copy(phase, target, part, own).wait_recv()

        def relay(part):
            await_line(OVER, part)
            line_copy(phase, BOTH, part).start()

        ready(SAME)
        take_fixed(phase, PEER)
        join((SAME, NEAR))
        for part in range(pieces):
            await_line(SIDE, part)
        ready(SIDE)
        relay(0)
        relay(1)
        join((SIDE, NEAR))
        relay(2)
        relay(3)
        ready(OVER, 0, 4 * piece)
        relay(4)
        relay(5)
        take_fixed(phase, ACROSS)
        fixed_copy(phase, ACROSS, PEER).start()
        ready(OVER, 4 * piece, 2 * piece)
        join((SAME, (ACROSS,)), (SIDE, (ACROSS,)), (OVER, NEAR + (ACROSS,)))
        take_fixed(phase, CORNER)
        join((SAME, (CORNER,)), (SIDE, (CORNER,)), (OVER, (CORNER,)))
        for part in range(pieces):
            await_line(BOTH, part)
        ready(BOTH)
        join((BOTH, ALL))
        for block in range(blocks):
            for which in (PEER, ACROSS, CORNER):
                closed_wait(phase, block, which)

    def turn(phase, target):
        turned[...] = landed[phase].reshape(tokens * SUB, channels).astype(jnp.float32)
        for row in range(rows):
            target[row] = turned[pl.ds(row, tokens, stride=SUB), :].astype(jnp.bfloat16)

    def finish(phase, own):
        for part in range(pieces):
            for target in (SIDE, OVER, BOTH):
                line_copy(phase, target, part, own).wait_send()
        for block in range(blocks):
            for which in (PEER, ACROSS, CORNER):
                closed_copy(phase, block, which, pl.ds(0, rows)).wait_send()
        fixed_copy(phase, OWN, PEER).wait_send()
        fixed_copy(phase, OWN, ACROSS).wait_send()
        fixed_copy(phase, ACROSS, PEER).wait_send()

    def send_line(phase, own, target):
        for part in range(pieces):
            line_copy(phase, target, part, own).start()

    late = jnp.logical_and(end, core == 0)

    def early_over(phase, own):
        send_line(phase, own, SIDE)

        @pl.when(jnp.logical_not(late))
        def _():
            send_line(phase, own, OVER)

    def launch(phase, own):
        fixed_copy(phase, OWN, ACROSS).start()
        fixed_copy(phase, OWN, PEER).start()

        @pl.when(late)
        def _():
            send_line(phase, own, OVER)

    def load(at):
        return pltpu.make_async_copy(inputs[at], copies[at], loaded.at[at])

    first_inputs = 3
    barrier = pltpu.get_barrier_semaphore()

    def greet(device):
        pl.semaphore_signal(barrier, inc=1, device_id={"axial": device}, device_id_type=MESH)

    for which in (PEER, ACROSS, CORNER):
        greet(mate(which))
    greet(device(SIDE, OWN))
    greet(device(OVER, OWN))
    for at in range(INPUTS):
        load(at).start()
    tri[...] = jnp.zeros_like(tri)
    normed_ref[...] = jnp.zeros_like(normed_ref)
    raw_ref[...] = jnp.zeros_like(raw_ref)
    split = 2 * hidden
    for at in range(first_inputs):
        load(at).wait()
    own_side(0, pair_ref[...], norm_out, proj_out[:, split:])
    pl.semaphore_wait(barrier, QUAD + 1)
    early_over(0, pair_ref)
    launch(0, pair_ref)
    for at in range(first_inputs, INPUTS):
        load(at).wait()
    exchange(0, pair_ref, norm_out, proj_out[:, :split], gate_out, mid_out, final_out)
    middle = held.at[1, SAME]
    turn(0, middle)
    early_over(1, middle)
    own_side(1, middle[...], norm_in, proj_in[:, :split])
    launch(1, middle)
    exchange(1, middle, norm_in, proj_in[:, split:], gate_in, mid_in, final_in)
    turn(1, out_ref)
    finish(0, pair_ref)
    finish(1, middle)


def gather_rows(devices, pair_rep, *weights):
    rows, tokens, channels = pair_rep.shape
    hidden = weights[1].shape[1] // 4
    gains = [w.reshape(1, -1) if w.ndim == 1 else w for w in weights]
    blocks = devices // QUAD
    pieces = PIECES
    block = (rows, tokens, hidden)
    low, full = jnp.bfloat16, jnp.float32
    return pl.pallas_call(
        functools.partial(line_kernel, devices, pieces),
        out_shape=jax.ShapeDtypeStruct(pair_rep.shape, pair_rep.dtype),
        in_specs=[pl.BlockSpec(memory_space=pl.ANY)] * INPUTS,
        out_specs=pl.BlockSpec(memory_space=pltpu.VMEM),
        scratch_shapes=[pltpu.VMEM(array.shape, array.dtype) for array in (pair_rep, *gains)]
        + [
            pltpu.SemaphoreType.DMA((INPUTS,)),
            pltpu.VMEM((2, blocks) + block, low),
            pltpu.VMEM((2, QUAD) + block, low),
            pltpu.VMEM((QUAD,) + block, full),
            pltpu.VMEM((blocks,) + block, full),
            pltpu.VMEM((rows, tokens + SUB, channels), full),
            pltpu.VMEM((rows, tokens + SUB, channels), full),
            pltpu.VMEM((blocks, rows, QUAD, SUB, channels), full),
            pltpu.VMEM((blocks, rows, QUAD, SUB, channels), full),
            pltpu.VMEM((blocks, rows, QUAD, SUB, channels), full),
            pltpu.VMEM((2, blocks, QUAD, rows, SUB, channels), low),
            pltpu.VMEM((2, devices, rows, SUB, channels), low),
            pltpu.VMEM((tokens * SUB, channels), full),
            pltpu.SemaphoreType.DMA((2, blocks, pieces)),
            pltpu.SemaphoreType.DMA((2, blocks, pieces)),
            pltpu.SemaphoreType.DMA((2, QUAD)),
            pltpu.SemaphoreType.DMA((2, QUAD)),
            pltpu.SemaphoreType.DMA((2, blocks, QUAD)),
            pltpu.SemaphoreType.DMA((2, devices)),
        ],
        compiler_params=pltpu.CompilerParams(
            collective_id=0, has_side_effects=True, vmem_limit_bytes=VMEM_BYTES
        ),
        name="gather_rows",
    )(pair_rep, *gains)


def exchange_channels(
    pair_rep,
    norm_out,
    proj_out,
    gate_out,
    mid_out,
    final_out,
    norm_in,
    proj_in,
    gate_in,
    mid_in,
    final_in,
):
    first = update(pair_rep, norm_out, proj_out, gate_out, mid_out, final_out, True)
    return update(first, norm_in, proj_in, gate_in, mid_in, final_in, False)


def solution(mesh):
    devices = mesh.shape["axial"]

    def on_device(*arrays):
        if fits(devices, arrays[0].shape, arrays[2].shape):
            return gather_rows(devices, *arrays)
        return exchange_channels(*arrays)

    placed = (P(("groups", "axial"), None, None), P(), P(), P(), P(), P(), P(), P(), P(), P(), P())
    return jax.shard_map(
        on_device,
        mesh=mesh,
        in_specs=placed,
        out_specs=P(("groups", "axial"), None, None),
        check_vma=False,
    )
```

```python
import functools

import jax
import jax.numpy as jnp
from jax import lax
from jax.experimental import pallas as pl
from jax.experimental.pallas import tpu as pltpu
from jax.sharding import PartitionSpec as P

EPS = 1e-05


def normalize(values, gain, axis):
    average = jnp.mean(values, axis=axis, keepdims=True)
    spread = jnp.mean(jnp.square(values - average), axis=axis, keepdims=True)
    return (values - average) * lax.rsqrt(spread + EPS) * gain


def channel_product(left_side, right_side, outgoing):
    formula = "kil,kjl->kij" if outgoing else "kli,klj->kij"
    got_left, got_right = (
        lax.all_to_all(left_side, "axial", split_axis=0, concat_axis=1, tiled=True),
        lax.all_to_all(right_side, "axial", split_axis=0, concat_axis=1, tiled=True),
    )
    return jnp.einsum(formula, got_left, got_right, preferred_element_type=jnp.float32)


def update(pair_rep, norm_gain, weights, gate_weight, mid_gain, final_weight, outgoing):
    normed = normalize(pair_rep.astype(jnp.float32), norm_gain, -1).astype(jnp.bfloat16)
    projected = jnp.einsum("rnc,ck->krn", normed, weights, preferred_element_type=jnp.float32)
    hidden = weights.shape[1] // 4
    left_side = (jax.nn.sigmoid(projected[hidden : 2 * hidden]) * projected[:hidden]).astype(
        jnp.bfloat16
    )
    right_side = (
        jax.nn.sigmoid(projected[3 * hidden :]) * projected[2 * hidden : 3 * hidden]
    ).astype(jnp.bfloat16)
    product = channel_product(left_side, right_side, outgoing)
    tri = lax.all_to_all(
        product.astype(jnp.bfloat16), "axial", split_axis=1, concat_axis=0, tiled=True
    )
    gating = jax.nn.sigmoid(
        jnp.einsum("rnc,ce->rne", normed, gate_weight, preferred_element_type=jnp.float32)
    )
    tri_normed = normalize(tri.astype(jnp.float32), mid_gain[:, None, None], 0).astype(jnp.bfloat16)
    result = jnp.einsum("krn,kc->rnc", tri_normed, final_weight, preferred_element_type=jnp.float32)
    return (pair_rep.astype(jnp.float32) + gating * result).astype(jnp.bfloat16)


MESH = pl.DeviceIdType.MESH
CORES = 2
SIDES = 2
QUAD = CORES * 2
SAME, SIDE, OVER, BOTH = range(4)
OWN, PEER, ACROSS, CORNER = range(4)
NEAR, FAR, ALL = (OWN, PEER), (ACROSS, CORNER), (OWN, PEER, ACROSS, CORNER)
SUB = 8
HALVES = 2
PAIR = 2
INPUTS = 11
PIECES = 6
STRIP_PIECES = 3
VMEM_BYTES = 56 * 1024 * 1024


def fits(devices, pair_shape, proj_shape):
    rows, tokens, channels = pair_shape
    hidden = proj_shape[1] // 4
    block = rows * tokens * hidden * 4
    return (
        devices == QUAD * SIDES * HALVES
        and devices * rows == tokens
        and rows <= SUB
        and rows % PIECES == 0
        and rows % PAIR == 0
        and rows % STRIP_PIECES == 0
        and tokens % (16 * HALVES) == 0
        and rows > SUB // 2
        and tokens % 16 == 0
        and channels == hidden
        and hidden % 128 == 0
        and (6 * (devices // QUAD) + 24) * block < VMEM_BYTES // 2
    )


def layer_norm(values, gain):
    average = jnp.mean(values, axis=-1, keepdims=True)
    centred = values - average
    spread = jnp.mean(jnp.square(centred), axis=-1, keepdims=True)
    return centred * lax.rsqrt(spread + EPS) * gain


def dot(left, right):
    return jnp.dot(left, right, preferred_element_type=jnp.float32)


def line_kernel(
    devices,
    pieces,
    *refs,
):
    inputs, out_ref, scratch = refs[:INPUTS], refs[INPUTS], refs[INPUTS + 1 :]
    copies, scratch = scratch[:INPUTS], scratch[INPUTS:]
    (
        pair_ref,
        norm_out,
        proj_out,
        gate_out,
        mid_out,
        final_out,
        norm_in,
        proj_in,
        gate_in,
        mid_in,
        final_in,
    ) = copies
    (
    loaded,
    held,
    fixed,
    strips,
    fixed_strips,
    fixed_f32,
    moving,
    normed_ref,
    raw_ref,
    resid,
    gating,
    tri,
    closed,
    landed,
    turned,
    line_send,
    line_recv,
    fixed_send,
    fixed_recv,
    closed_send,
    closed_recv,
    strip_send,
    strip_recv,
    fixed_strip_send,
    fixed_strip_recv,
    ) = scratch
    rows, tokens, channels = pair_ref.shape
    hidden = fixed.shape[-1]
    blocks = devices // QUAD
    piece = rows // pieces
    me = lax.axis_index("axial")
    core = me % CORES
    side = (me // CORES) % SIDES
    level = me // (CORES * SIDES)
    half, floor = level // 2, level % 2
    end = jnp.logical_or(level == 0, level == 2 * HALVES - 1)
    places = ((0, 0), (0, 1), (1, 0), (1, 1))
    seats = ((0, 0), (0, 1), (1, 1), (1, 0))

    def turned_to(value, flip):
        return 1 - value if flip else value

    def device(block, which):
        over, aside = places[block]
        up, swap = seats[which]
        at = 2 * turned_to(half, over) + turned_to(floor, up)
        return (at * SIDES + turned_to(side, aside)) * CORES + turned_to(core, swap != aside)

    def mate(which):
        return device(SAME, which)

    def remote(source, target, sent, got, device):
        return pltpu.make_async_remote_copy(
            src_ref=source,
            dst_ref=target,
            send_sem=sent,
            recv_sem=got,
            device_id={"axial": device},
            device_id_type=MESH,
        )

    def window(part):
        return pl.ds(part * piece, piece)

    def line_copy(phase, target, part, source=None):
        came = held.at[phase, OVER, window(part)]
        goes = came if target == BOTH else source.at[window(part)]
        return remote(
            goes,
            held.at[phase, target, window(part)],
            line_send.at[phase, target, part],
            line_recv.at[phase, target, part],
            device(OVER if target == OVER else SIDE, OWN),
        )

    def fixed_copy(phase, which, to):
        arrives = {(OWN, PEER): PEER, (OWN, ACROSS): ACROSS, (ACROSS, PEER): CORNER}[which, to]
        return remote(
            fixed.at[phase, which],
            fixed.at[phase, arrives],
            fixed_send.at[phase, arrives],
            fixed_recv.at[phase, arrives],
            mate(to),
        )

    def closed_copy(phase, block, which, span):
        here = device(block, OWN)
        return remote(
            closed.at[phase, block, which, span, pl.ds(0, rows)],
            landed.at[phase, here, span, pl.ds(0, rows)],
            closed_send.at[phase, block, which],
            closed_recv.at[phase, here],
            mate(which),
        )

    def closed_wait(phase, block, which):
        there = device(block, which)
        remote(
            closed.at[phase, block, which, :, pl.ds(0, rows)],
            landed.at[phase, there, :, pl.ds(0, rows)],
            closed_send.at[phase, block, which],
            closed_recv.at[phase, there],
            mate(which),
        ).wait_recv()

    width = tokens // HALVES
    thick = rows // STRIP_PIECES

    def strip_copy(target, chunk, part):
        span = pl.ds(part * thick, thick)
        lands = 1 - chunk if target == OVER else chunk
        return remote(
            strips.at[OVER if target == BOTH else SAME, chunk, span],
            strips.at[target, lands, span],
            strip_send.at[target, chunk, part],
            strip_recv.at[target, lands, part],
            device(OVER if target == OVER else SIDE, OWN),
        )

    def strip_wait(target, chunk, part):
        strip_copy(target, 1 - chunk if target == OVER else chunk, part).wait_recv()

    def fixed_strip_copy(which, to, chunk):
        arrives = {(OWN, PEER): PEER, (OWN, ACROSS): ACROSS, (ACROSS, PEER): CORNER}[which, to]
        return remote(
            fixed_strips.at[which, chunk],
            fixed_strips.at[arrives, chunk],
            fixed_strip_send.at[arrives, chunk],
            fixed_strip_recv.at[arrives, chunk],
            mate(to),
        )

    def columns(chunk):
        return slice(chunk * width, (chunk + 1) * width)

    def send_strip(chunk):
        for part in range(STRIP_PIECES):
            strip_copy(OVER, chunk, part).start()
            strip_copy(SIDE, chunk, part).start()

    def relay_strip(chunk, part):
        strip_wait(OVER, chunk, part)
        strip_copy(BOTH, chunk, part).start()

    def await_strip(target, chunk):
        for part in range(STRIP_PIECES):
            strip_wait(target, chunk, part)

    def take_fixed_strip(which, chunk):
        source = ACROSS if which == CORNER else OWN
        fixed_strip_copy(source, ACROSS if which == ACROSS else PEER, chunk).wait_recv()
        fixed_f32[which, :, columns(chunk), :] = fixed_strips[which, chunk].astype(jnp.float32)

    def own_strip(chunk, norm, weights):
        values = flat(strips[SAME, chunk]).astype(jnp.float32)
        normed = layer_norm(values, norm[...]).astype(jnp.bfloat16)
        made = gated(dot(normed, weights)).reshape(rows, width, hidden)
        fixed_strips[OWN, chunk] = made
        fixed_f32[OWN, :, columns(chunk), :] = made.astype(jnp.float32)
        fixed_strip_copy(OWN, ACROSS, chunk).start()
        fixed_strip_copy(OWN, PEER, chunk).start()

    def turn_strip(chunk):
        group = devices // HALVES
        base = (half if chunk == 0 else 1 - half) * group
        size = group * rows * SUB
        picked = landed[0, pl.ds(base, group)].reshape(size, channels)
        turned[:size] = picked.astype(jnp.float32)
        for row in range(rows):
            taken = turned[pl.ds(row, width, stride=SUB), :]
            strips[SAME, chunk, row] = taken.astype(jnp.bfloat16)

    def flat(values):
        return values.reshape(-1, values.shape[-1])

    def gated(projected):
        return (jax.nn.sigmoid(projected[:, hidden:]) * projected[:, :hidden]).astype(jnp.bfloat16)

    def own_side(phase, block, norm, weights):
        normed = layer_norm(flat(block).astype(jnp.float32), norm[...]).astype(jnp.bfloat16)
        made = gated(dot(normed, weights)).reshape(rows, tokens, hidden)
        fixed[phase, OWN] = made
        fixed_f32[OWN] = made.astype(jnp.float32)

    def take_fixed(phase, which):
        source = ACROSS if which == CORNER else OWN
        fixed_copy(phase, source, ACROSS if which == ACROSS else PEER).wait_recv()
        fixed_f32[which] = fixed[phase, which].astype(jnp.float32)

    def prepare(phase, source, block, first, count, norm, weights, gate):
        span = pl.ds(first, count)
        raw = source[span].astype(jnp.float32)
        normed = layer_norm(flat(raw), norm[...])
        raw_ref[:count, :tokens] = raw
        normed_ref[:count, :tokens] = normed.reshape(count, tokens, channels)
        made = gated(dot(normed.astype(jnp.bfloat16), weights))
        moving[block, span] = made.astype(jnp.float32).reshape(count, tokens, hidden)
        picked = []
        for row in range(count):
            for which in range(QUAD):
                at = pl.ds(mate(which) * rows, SUB)
                picked.append(normed_ref[row, at, :])
                resid[block, first + row, which] = raw_ref[row, at, :]
        picked = jnp.concatenate(picked, axis=0).astype(jnp.bfloat16)
        opened = jax.nn.sigmoid(dot(picked, gate[...]))
        gating[block, span] = opened.reshape(count, QUAD, SUB, channels)

    def prepare_strip(block, chunk, norm, weights, gate):
        raw = strips[block, chunk].astype(jnp.float32)
        normed = layer_norm(flat(raw), norm[...])
        made = gated(dot(normed.astype(jnp.bfloat16), weights))
        made = made.astype(jnp.float32).reshape(rows, width, hidden)
        moving[block, :, columns(chunk), :] = made
        if chunk:
            return
        raw_ref[:, :width] = raw
        normed_ref[:, :width] = normed.reshape(rows, width, channels)
        picked = []
        for row in range(rows):
            for which in range(QUAD):
                at = pl.ds((mate(which) - half * (devices // HALVES)) * rows, SUB)
                picked.append(normed_ref[row, at, :])
                resid[block, row, which] = raw_ref[row, at, :]
        picked = jnp.concatenate(picked, axis=0).astype(jnp.bfloat16)
        opened = jax.nn.sigmoid(dot(picked, gate[...]))
        gating[block] = opened.reshape(rows, QUAD, SUB, channels)

    def fold(parts):
        place = lax.broadcasted_iota(jnp.int32, (SUB, hidden), 0)
        apart = SUB // 2
        while apart:
            first_half = (place // apart) % 2 == 0

            def joined(low, high):
                ahead = low + pltpu.roll(low, SUB - apart, 0)
                if high is None:
                    return jnp.where(first_half, ahead, low + pltpu.roll(low, apart, 0))
                return jnp.where(first_half, ahead, high + pltpu.roll(high, apart, 0))

            parts = parts + [None] * (2 * apart - len(parts))
            parts = [joined(parts[at], parts[at + apart]) for at in range(apart)]
            apart //= 2
        return parts[0]

    def tiles(values):
        return values.reshape(tokens // SUB, SUB, hidden)

    def multiply(jobs):
        def one(at, carry):
            for block, group in jobs:
                right = [tiles(moving[block, PAIR * at + row]) for row in range(PAIR)]
                for which in group:
                    sums = [[], []]
                    for own in range(rows):
                        left = tiles(fixed_f32[which, own])
                        for row in range(PAIR):
                            sums[row].append(jnp.sum(left * right[row], axis=0))
                    for row in range(PAIR):
                        tri[block, PAIR * at + row, which] = fold(sums[row])
            return carry

        lax.fori_loop(0, rows // PAIR, one, 0)

    def close(phase, jobs, mid, final):
        multiply([(block, group) for block, _, _, group in jobs])

        def gather(ref):
            picked = []
            for block, first, count, group in jobs:
                lanes = slice(group[0], group[-1] + 1)
                picked.append(flat(ref[block, first : first + count, lanes]))
            return jnp.concatenate(picked, axis=0) if len(picked) > 1 else picked[0]

        product = gather(tri).astype(jnp.bfloat16).astype(jnp.float32)
        normed = layer_norm(product, mid[...]).astype(jnp.bfloat16)
        result = gather(resid) + gather(gating) * dot(normed, final[...])
        result = result.astype(jnp.bfloat16)
        at = 0
        for block, first, count, group in jobs:
            size = count * len(group) * SUB
            part = result[at : at + size].reshape(count, len(group), SUB, channels)
            at += size
            span = pl.ds(first, count)
            for place, which in enumerate(group):
                if which == OWN:
                    landed[phase, device(block, OWN), span] = part[:, place]
                else:
                    closed[phase, block, which, span] = part[:, place]
        for block, first, count, group in jobs:
            for which in group:
                if which != OWN:
                    closed_copy(phase, block, which, pl.ds(first, count)).start()

    def exchange(phase, own, norm, weights, gate, mid, final):
        def ready(block, first=0, count=rows):
            source = own if block == SAME else held.at[phase, block]
            prepare(phase, source, block, first, count, norm, weights, gate)

        def join(*jobs):
            close(phase, [(block, 0, rows, group) for block, group in jobs], mid, final)

        def await_line(target, part):
            line_copy(phase, target, part, own).wait_recv()

        def relay(part):
            await_line(OVER, part)
            line_copy(phase, BOTH, part).start()

        def await_all(target):
            for part in range(pieces):
                await_line(target, part)

        def take_across():
            take_fixed(phase, ACROSS)
            fixed_copy(phase, ACROSS, PEER).start()

        def hand_on():
            landed_wait(phase, (SAME, SIDE))
            turn_strip(0)
            send_strip(0)

        ready(SAME)
        take_fixed(phase, PEER)
        join((SAME, NEAR))

        @pl.when(end)
        def _():
            take_across()
            await_all(SIDE)
            ready(SIDE)
            join((SAME, (ACROSS,)), (SIDE, NEAR + (ACROSS,)))
            relay(0)
            relay(1)
            take_fixed(phase, CORNER)
            join((SAME, (CORNER,)), (SIDE, (CORNER,)))
            relay(2)
            relay(3)
            ready(OVER, 0, 4 * piece)
            relay(4)
            relay(5)
            ready(OVER, 4 * piece, 2 * piece)
            join((OVER, ALL))
            await_all(BOTH)
            ready(BOTH)
            join((BOTH, FAR))
            hand_on()
            join((BOTH, NEAR))

        @pl.when(jnp.logical_not(end))
        def _():
            fixed_copy(phase, OWN, ACROSS).wait_send()
            send_line(phase, own, OVER)
            for part in range(pieces):
                relay(part)
            ready(OVER)
            join((OVER, NEAR))
            await_all(SIDE)
            ready(SIDE)
            join((SIDE, NEAR))
            take_across()
            join((SAME, (ACROSS,)), (SIDE, (ACROSS,)))
            await_all(BOTH)
            ready(BOTH)
            take_fixed(phase, CORNER)
            join((SAME, (CORNER,)), (SIDE, (CORNER,)))
            join((OVER, FAR), (BOTH, FAR))
            hand_on()
            join((BOTH, NEAR))

    def landed_wait(phase, picked):
        for block in picked:
            for which in (PEER, ACROSS, CORNER):
                closed_wait(phase, block, which)

    def exchange_strips(norm, own_weights, weights, gate, mid, final):
        def ready(block, chunk):
            prepare_strip(block, chunk, norm, weights, gate)

        def join(*jobs):
            close(1, [(block, 0, rows, group) for block, group in jobs], mid, final)

        own_strip(0, norm, own_weights)
        ready(SAME, 0)
        landed_wait(0, (OVER, BOTH))
        turn_strip(1)
        send_strip(1)
        own_strip(1, norm, own_weights)
        ready(SAME, 1)
        for chunk in range(HALVES):
            take_fixed_strip(PEER, chunk)
        join((SAME, NEAR))
        for part in range(STRIP_PIECES):
            relay_strip(1, part)
        await_strip(SIDE, 0)
        ready(SIDE, 0)
        ready(OVER, 1)
        await_strip(SIDE, 1)
        ready(SIDE, 1)
        join((SIDE, NEAR))
        relay_strip(0, 0)
        for chunk in range(HALVES):
            take_fixed_strip(ACROSS, chunk)
            fixed_strip_copy(ACROSS, PEER, chunk).start()
        relay_strip(0, 1)
        join((SAME, (ACROSS,)), (SIDE, (ACROSS,)))
        relay_strip(0, 2)
        ready(OVER, 0)
        await_strip(BOTH, 1)
        ready(BOTH, 1)
        for chunk in range(HALVES):
            take_fixed_strip(CORNER, chunk)
        join((SAME, (CORNER,)), (SIDE, (CORNER,)), (OVER, ALL))
        await_strip(BOTH, 0)
        ready(BOTH, 0)
        join((BOTH, FAR))
        join((BOTH, NEAR))
        landed_wait(1, (SAME, SIDE, OVER, BOTH))

    def turn(phase, target):
        turned[...] = landed[phase].reshape(tokens * SUB, channels).astype(jnp.float32)
        for row in range(rows):
            target[row] = turned[pl.ds(row, tokens, stride=SUB), :].astype(jnp.bfloat16)

    def finish(phase, own):
        for part in range(pieces):
            for target in (SIDE, OVER, BOTH):
                line_copy(phase, target, part, own).wait_send()
        fixed_copy(phase, OWN, PEER).wait_send()

        @pl.when(end)
        def _():
            fixed_copy(phase, OWN, ACROSS).wait_send()

        fixed_copy(phase, ACROSS, PEER).wait_send()
        finish_closed(phase)

    def finish_closed(phase):
        for block in range(blocks):
            for which in (PEER, ACROSS, CORNER):
                closed_copy(phase, block, which, pl.ds(0, rows)).wait_send()

    def send_line(phase, own, target):
        for part in range(pieces):
            line_copy(phase, target, part, own).start()

    def early_over(phase, own):
        send_line(phase, own, SIDE)

        @pl.when(end)
        def _():
            send_line(phase, own, OVER)

    def launch(phase, own):
        fixed_copy(phase, OWN, ACROSS).start()
        fixed_copy(phase, OWN, PEER).start()

    def load(at):
        return pltpu.make_async_copy(inputs[at], copies[at], loaded.at[at])

    first_inputs = 3
    barrier = pltpu.get_barrier_semaphore()

    def greet(device):
        pl.semaphore_signal(barrier, inc=1, device_id={"axial": device}, device_id_type=MESH)

    for which in (PEER, ACROSS, CORNER):
        greet(mate(which))
    greet(device(SIDE, OWN))
    greet(device(OVER, OWN))
    for at in range(INPUTS):
        load(at).start()
    tri[...] = jnp.zeros_like(tri)
    normed_ref[...] = jnp.zeros_like(normed_ref)
    raw_ref[...] = jnp.zeros_like(raw_ref)
    split = 2 * hidden
    for at in range(first_inputs):
        load(at).wait()
    own_side(0, pair_ref[...], norm_out, proj_out[:, split:])
    pl.semaphore_wait(barrier, QUAD + 1)
    early_over(0, pair_ref)
    launch(0, pair_ref)
    for at in range(first_inputs, INPUTS):
        load(at).wait()
    exchange(0, pair_ref, norm_out, proj_out[:, :split], gate_out, mid_out, final_out)
    exchange_strips(norm_in, proj_in[:, :split], proj_in[:, split:], gate_in, mid_in, final_in)
    turn(1, out_ref)
    finish(0, pair_ref)
    for chunk in range(HALVES):
        for part in range(STRIP_PIECES):
            for target in (SIDE, OVER, BOTH):
                strip_copy(target, chunk, part).wait_send()
        fixed_strip_copy(OWN, PEER, chunk).wait_send()
        fixed_strip_copy(OWN, ACROSS, chunk).wait_send()
        fixed_strip_copy(ACROSS, PEER, chunk).wait_send()
    finish_closed(1)


def gather_rows(devices, pair_rep, *weights):
    rows, tokens, channels = pair_rep.shape
    hidden = weights[1].shape[1] // 4
    gains = [w.reshape(1, -1) if w.ndim == 1 else w for w in weights]
    blocks = devices // QUAD
    pieces = PIECES
    block = (rows, tokens, hidden)
    low, full = jnp.bfloat16, jnp.float32
    return pl.pallas_call(
        functools.partial(line_kernel, devices, pieces),
        out_shape=jax.ShapeDtypeStruct(pair_rep.shape, pair_rep.dtype),
        in_specs=[pl.BlockSpec(memory_space=pl.ANY)] * INPUTS,
        out_specs=pl.BlockSpec(memory_space=pltpu.VMEM),
        scratch_shapes=[pltpu.VMEM(array.shape, array.dtype) for array in (pair_rep, *gains)]
        + [
            pltpu.SemaphoreType.DMA((INPUTS,)),
            pltpu.VMEM((1, blocks) + block, low),
            pltpu.VMEM((1, QUAD) + block, low),
            pltpu.VMEM((blocks, HALVES, rows, tokens // HALVES, channels), low),
            pltpu.VMEM((QUAD, HALVES, rows, tokens // HALVES, hidden), low),
            pltpu.VMEM((QUAD,) + block, full),
            pltpu.VMEM((blocks,) + block, full),
            pltpu.VMEM((rows, tokens + SUB, channels), full),
            pltpu.VMEM((rows, tokens + SUB, channels), full),
            pltpu.VMEM((blocks, rows, QUAD, SUB, channels), full),
            pltpu.VMEM((blocks, rows, QUAD, SUB, channels), full),
            pltpu.VMEM((blocks, rows, QUAD, SUB, channels), full),
            pltpu.VMEM((2, blocks, QUAD, rows, SUB, channels), low),
            pltpu.VMEM((2, devices, rows, SUB, channels), low),
            pltpu.VMEM((tokens * SUB, channels), full),
            pltpu.SemaphoreType.DMA((2, blocks, pieces)),
            pltpu.SemaphoreType.DMA((2, blocks, pieces)),
            pltpu.SemaphoreType.DMA((2, QUAD)),
            pltpu.SemaphoreType.DMA((2, QUAD)),
            pltpu.SemaphoreType.DMA((2, blocks, QUAD)),
            pltpu.SemaphoreType.DMA((2, devices)),
            pltpu.SemaphoreType.DMA((blocks, HALVES, STRIP_PIECES)),
            pltpu.SemaphoreType.DMA((blocks, HALVES, STRIP_PIECES)),
            pltpu.SemaphoreType.DMA((QUAD, HALVES)),
            pltpu.SemaphoreType.DMA((QUAD, HALVES)),
        ],
        compiler_params=pltpu.CompilerParams(
            collective_id=0, has_side_effects=True, vmem_limit_bytes=VMEM_BYTES
        ),
        name="gather_rows",
    )(pair_rep, *gains)


def exchange_channels(
    pair_rep,
    norm_out,
    proj_out,
    gate_out,
    mid_out,
    final_out,
    norm_in,
    proj_in,
    gate_in,
    mid_in,
    final_in,
):
    first = update(pair_rep, norm_out, proj_out, gate_out, mid_out, final_out, True)
    return update(first, norm_in, proj_in, gate_in, mid_in, final_in, False)


def solution(mesh):
    devices = mesh.shape["axial"]

    def on_device(*arrays):
        if fits(devices, arrays[0].shape, arrays[2].shape):
            return gather_rows(devices, *arrays)
        return exchange_channels(*arrays)

    placed = (P(("groups", "axial"), None, None), P(), P(), P(), P(), P(), P(), P(), P(), P(), P())
    return jax.shard_map(
        on_device,
        mesh=mesh,
        in_specs=placed,
        out_specs=P(("groups", "axial"), None, None),
        check_vma=False,
    )
```

```python
import functools

import jax
import jax.numpy as jnp
from jax import lax
from jax.experimental import pallas as pl
from jax.experimental.pallas import tpu as pltpu
from jax.sharding import PartitionSpec as P

EPS = 1e-05


def normalize(values, gain, axis):
    average = jnp.mean(values, axis=axis, keepdims=True)
    spread = jnp.mean(jnp.square(values - average), axis=axis, keepdims=True)
    return (values - average) * lax.rsqrt(spread + EPS) * gain


def channel_product(left_side, right_side, outgoing):
    formula = "kil,kjl->kij" if outgoing else "kli,klj->kij"
    got_left, got_right = (
        lax.all_to_all(left_side, "axial", split_axis=0, concat_axis=1, tiled=True),
        lax.all_to_all(right_side, "axial", split_axis=0, concat_axis=1, tiled=True),
    )
    return jnp.einsum(formula, got_left, got_right, preferred_element_type=jnp.float32)


def update(pair_rep, norm_gain, weights, gate_weight, mid_gain, final_weight, outgoing):
    normed = normalize(pair_rep.astype(jnp.float32), norm_gain, -1).astype(jnp.bfloat16)
    projected = jnp.einsum("rnc,ck->krn", normed, weights, preferred_element_type=jnp.float32)
    hidden = weights.shape[1] // 4
    left_side = (jax.nn.sigmoid(projected[hidden : 2 * hidden]) * projected[:hidden]).astype(
        jnp.bfloat16
    )
    right_side = (
        jax.nn.sigmoid(projected[3 * hidden :]) * projected[2 * hidden : 3 * hidden]
    ).astype(jnp.bfloat16)
    product = channel_product(left_side, right_side, outgoing)
    tri = lax.all_to_all(
        product.astype(jnp.bfloat16), "axial", split_axis=1, concat_axis=0, tiled=True
    )
    gating = jax.nn.sigmoid(
        jnp.einsum("rnc,ce->rne", normed, gate_weight, preferred_element_type=jnp.float32)
    )
    tri_normed = normalize(tri.astype(jnp.float32), mid_gain[:, None, None], 0).astype(jnp.bfloat16)
    result = jnp.einsum("krn,kc->rnc", tri_normed, final_weight, preferred_element_type=jnp.float32)
    return (pair_rep.astype(jnp.float32) + gating * result).astype(jnp.bfloat16)


MESH = pl.DeviceIdType.MESH
CORES = 2
SIDES = 2
QUAD = CORES * 2
SAME, SIDE, OVER, BOTH = range(4)
OWN, PEER, ACROSS, CORNER = range(4)
NEAR, FAR, ALL = (OWN, PEER), (ACROSS, CORNER), (OWN, PEER, ACROSS, CORNER)
SUB = 8
HALVES = 2
PAIR = 2
INPUTS = 11
PIECES = 6
STRIP_PIECES = 3
VMEM_BYTES = 56 * 1024 * 1024


def fits(devices, pair_shape, proj_shape):
    rows, tokens, channels = pair_shape
    hidden = proj_shape[1] // 4
    block = rows * tokens * hidden * 4
    return (
        devices == QUAD * SIDES * HALVES
        and devices * rows == tokens
        and rows <= SUB
        and rows % PIECES == 0
        and rows % PAIR == 0
        and rows % STRIP_PIECES == 0
        and tokens % (16 * HALVES) == 0
        and rows > SUB // 2
        and tokens % 16 == 0
        and channels == hidden
        and hidden % 128 == 0
        and (6 * (devices // QUAD) + 24) * block < VMEM_BYTES // 2
    )


def layer_norm(values, gain):
    average = jnp.mean(values, axis=-1, keepdims=True)
    centred = values - average
    spread = jnp.mean(jnp.square(centred), axis=-1, keepdims=True)
    return centred * lax.rsqrt(spread + EPS) * gain


def dot(left, right):
    return jnp.dot(left, right, preferred_element_type=jnp.float32)


def line_kernel(
    devices,
    pieces,
    *refs,
):
    inputs, out_ref, scratch = refs[:INPUTS], refs[INPUTS], refs[INPUTS + 1 :]
    copies, scratch = scratch[:INPUTS], scratch[INPUTS:]
    (
        pair_ref,
        norm_out,
        proj_out,
        gate_out,
        mid_out,
        final_out,
        norm_in,
        proj_in,
        gate_in,
        mid_in,
        final_in,
    ) = copies
    (
    loaded,
    held,
    fixed,
    strips,
    fixed_strips,
    fixed_f32,
    moving,
    normed_ref,
    raw_ref,
    resid,
    gating,
    tri,
    closed,
    landed,
    turned,
    line_send,
    line_recv,
    fixed_send,
    fixed_recv,
    closed_send,
    closed_recv,
    strip_send,
    strip_recv,
    fixed_strip_send,
    fixed_strip_recv,
    ) = scratch
    rows, tokens, channels = pair_ref.shape
    hidden = fixed.shape[-1]
    blocks = devices // QUAD
    piece = rows // pieces
    me = lax.axis_index("axial")
    core = me % CORES
    side = (me // CORES) % SIDES
    level = me // (CORES * SIDES)
    half, floor = level // 2, level % 2
    end = jnp.logical_or(level == 0, level == 2 * HALVES - 1)
    places = ((0, 0), (0, 1), (1, 0), (1, 1))
    seats = ((0, 0), (0, 1), (1, 1), (1, 0))

    def turned_to(value, flip):
        return 1 - value if flip else value

    def device(block, which):
        over, aside = places[block]
        up, swap = seats[which]
        at = 2 * turned_to(half, over) + turned_to(floor, up)
        return (at * SIDES + turned_to(side, aside)) * CORES + turned_to(core, swap != aside)

    def mate(which):
        return device(SAME, which)

    def remote(source, target, sent, got, device):
        return pltpu.make_async_remote_copy(
            src_ref=source,
            dst_ref=target,
            send_sem=sent,
            recv_sem=got,
            device_id={"axial": device},
            device_id_type=MESH,
        )

    def window(part):
        return pl.ds(part * piece, piece)

    def line_copy(phase, target, part, source=None):
        came = held.at[phase, OVER, window(part)]
        goes = came if target == BOTH else source.at[window(part)]
        return remote(
            goes,
            held.at[phase, target, window(part)],
            line_send.at[phase, target, part],
            line_recv.at[phase, target, part],
            device(OVER if target == OVER else SIDE, OWN),
        )

    def fixed_copy(phase, which, to):
        arrives = {(OWN, PEER): PEER, (OWN, ACROSS): ACROSS, (ACROSS, PEER): CORNER}[which, to]
        return remote(
            fixed.at[phase, which],
            fixed.at[phase, arrives],
            fixed_send.at[phase, arrives],
            fixed_recv.at[phase, arrives],
            mate(to),
        )

    def closed_copy(phase, block, which, span):
        here = device(block, OWN)
        return remote(
            closed.at[phase, block, which, span, pl.ds(0, rows)],
            landed.at[phase, here, span, pl.ds(0, rows)],
            closed_send.at[phase, block, which],
            closed_recv.at[phase, here],
            mate(which),
        )

    def closed_wait(phase, block, which):
        there = device(block, which)
        remote(
            closed.at[phase, block, which, :, pl.ds(0, rows)],
            landed.at[phase, there, :, pl.ds(0, rows)],
            closed_send.at[phase, block, which],
            closed_recv.at[phase, there],
            mate(which),
        ).wait_recv()

    width = tokens // HALVES
    thick = rows // STRIP_PIECES

    def strip_copy(target, chunk, part):
        span = pl.ds(part * thick, thick)
        lands = 1 - chunk if target == OVER else chunk
        return remote(
            strips.at[OVER if target == BOTH else SAME, chunk, span],
            strips.at[target, lands, span],
            strip_send.at[target, chunk, part],
            strip_recv.at[target, lands, part],
            device(OVER if target == OVER else SIDE, OWN),
        )

    def strip_wait(target, chunk, part):
        strip_copy(target, 1 - chunk if target == OVER else chunk, part).wait_recv()

    def fixed_strip_copy(which, to, chunk):
        arrives = {(OWN, PEER): PEER, (OWN, ACROSS): ACROSS, (ACROSS, PEER): CORNER}[which, to]
        return remote(
            fixed_strips.at[which, chunk],
            fixed_strips.at[arrives, chunk],
            fixed_strip_send.at[arrives, chunk],
            fixed_strip_recv.at[arrives, chunk],
            mate(to),
        )

    def columns(chunk):
        return slice(chunk * width, (chunk + 1) * width)

    def send_strip(chunk):
        for part in range(STRIP_PIECES):
            strip_copy(OVER, chunk, part).start()
            strip_copy(SIDE, chunk, part).start()

    def relay_strip(chunk, part):
        strip_wait(OVER, chunk, part)
        strip_copy(BOTH, chunk, part).start()

    def await_strip(target, chunk):
        for part in range(STRIP_PIECES):
            strip_wait(target, chunk, part)

    def take_fixed_strip(which, chunk):
        source = ACROSS if which == CORNER else OWN
        fixed_strip_copy(source, ACROSS if which == ACROSS else PEER, chunk).wait_recv()
        fixed_f32[which, :, columns(chunk), :] = fixed_strips[which, chunk].astype(jnp.float32)

    def own_strip(chunk, norm, weights):
        values = flat(strips[SAME, chunk]).astype(jnp.float32)
        normed = layer_norm(values, norm[...]).astype(jnp.bfloat16)
        made = gated(dot(normed, weights)).reshape(rows, width, hidden)
        fixed_strips[OWN, chunk] = made
        fixed_f32[OWN, :, columns(chunk), :] = made.astype(jnp.float32)
        fixed_strip_copy(OWN, ACROSS, chunk).start()
        fixed_strip_copy(OWN, PEER, chunk).start()

    def turn_strip(chunk):
        group = devices // HALVES
        base = (half if chunk == 0 else 1 - half) * group
        size = group * rows * SUB
        picked = landed[0, pl.ds(base, group)].reshape(size, channels)
        turned[:size] = picked.astype(jnp.float32)
        for row in range(rows):
            taken = turned[pl.ds(row, width, stride=SUB), :]
            strips[SAME, chunk, row] = taken.astype(jnp.bfloat16)

    def flat(values):
        return values.reshape(-1, values.shape[-1])

    def gated(projected):
        return (jax.nn.sigmoid(projected[:, hidden:]) * projected[:, :hidden]).astype(jnp.bfloat16)

    def own_side(phase, block, norm, weights):
        normed = layer_norm(flat(block).astype(jnp.float32), norm[...]).astype(jnp.bfloat16)
        made = gated(dot(normed, weights)).reshape(rows, tokens, hidden)
        fixed[phase, OWN] = made
        fixed_f32[OWN] = made.astype(jnp.float32)

    def take_fixed(phase, which):
        source = ACROSS if which == CORNER else OWN
        fixed_copy(phase, source, ACROSS if which == ACROSS else PEER).wait_recv()
        fixed_f32[which] = fixed[phase, which].astype(jnp.float32)

    def prepare(phase, source, block, first, count, norm, weights, gate):
        span = pl.ds(first, count)
        raw = source[span].astype(jnp.float32)
        normed = layer_norm(flat(raw), norm[...])
        raw_ref[:count, :tokens] = raw
        normed_ref[:count, :tokens] = normed.reshape(count, tokens, channels)
        made = gated(dot(normed.astype(jnp.bfloat16), weights))
        moving[block, span] = made.astype(jnp.float32).reshape(count, tokens, hidden)
        picked = []
        for row in range(count):
            for which in range(QUAD):
                at = pl.ds(mate(which) * rows, SUB)
                picked.append(normed_ref[row, at, :])
                resid[block, first + row, which] = raw_ref[row, at, :]
        picked = jnp.concatenate(picked, axis=0).astype(jnp.bfloat16)
        opened = jax.nn.sigmoid(dot(picked, gate[...]))
        gating[block, span] = opened.reshape(count, QUAD, SUB, channels)

    def prepare_strip(block, chunk, norm, weights, gate):
        raw = strips[block, chunk].astype(jnp.float32)
        normed = layer_norm(flat(raw), norm[...])
        made = gated(dot(normed.astype(jnp.bfloat16), weights))
        made = made.astype(jnp.float32).reshape(rows, width, hidden)
        moving[block, :, columns(chunk), :] = made
        if chunk:
            return
        raw_ref[:, :width] = raw
        normed_ref[:, :width] = normed.reshape(rows, width, channels)
        picked = []
        for row in range(rows):
            for which in range(QUAD):
                at = pl.ds((mate(which) - half * (devices // HALVES)) * rows, SUB)
                picked.append(normed_ref[row, at, :])
                resid[block, row, which] = raw_ref[row, at, :]
        picked = jnp.concatenate(picked, axis=0).astype(jnp.bfloat16)
        opened = jax.nn.sigmoid(dot(picked, gate[...]))
        gating[block] = opened.reshape(rows, QUAD, SUB, channels)

    def fold(parts):
        place = lax.broadcasted_iota(jnp.int32, (SUB, hidden), 0)
        apart = SUB // 2
        while apart:
            first_half = (place // apart) % 2 == 0

            def joined(low, high):
                ahead = low + pltpu.roll(low, SUB - apart, 0)
                if high is None:
                    return jnp.where(first_half, ahead, low + pltpu.roll(low, apart, 0))
                return jnp.where(first_half, ahead, high + pltpu.roll(high, apart, 0))

            parts = parts + [None] * (2 * apart - len(parts))
            parts = [joined(parts[at], parts[at + apart]) for at in range(apart)]
            apart //= 2
        return parts[0]

    def tiles(values):
        return values.reshape(tokens // SUB, SUB, hidden)

    def multiply(jobs):
        def one(at, carry):
            for block, group in jobs:
                right = [tiles(moving[block, PAIR * at + row]) for row in range(PAIR)]
                for which in group:
                    sums = [[], []]
                    for own in range(rows):
                        left = tiles(fixed_f32[which, own])
                        for row in range(PAIR):
                            sums[row].append(jnp.sum(left * right[row], axis=0))
                    for row in range(PAIR):
                        tri[block, PAIR * at + row, which] = fold(sums[row])
            return carry

        lax.fori_loop(0, rows // PAIR, one, 0)

    def close(phase, jobs, mid, final):
        multiply([(block, group) for block, _, _, group in jobs])

        def gather(ref):
            picked = []
            for block, first, count, group in jobs:
                lanes = slice(group[0], group[-1] + 1)
                picked.append(flat(ref[block, first : first + count, lanes]))
            return jnp.concatenate(picked, axis=0) if len(picked) > 1 else picked[0]

        product = gather(tri).astype(jnp.bfloat16).astype(jnp.float32)
        normed = layer_norm(product, mid[...]).astype(jnp.bfloat16)
        result = gather(resid) + gather(gating) * dot(normed, final[...])
        result = result.astype(jnp.bfloat16)
        at = 0
        for block, first, count, group in jobs:
            size = count * len(group) * SUB
            part = result[at : at + size].reshape(count, len(group), SUB, channels)
            at += size
            span = pl.ds(first, count)
            for place, which in enumerate(group):
                if which == OWN:
                    landed[phase, device(block, OWN), span] = part[:, place]
                else:
                    closed[phase, block, which, span] = part[:, place]
        for block, first, count, group in jobs:
            for which in group:
                if which != OWN:
                    closed_copy(phase, block, which, pl.ds(first, count)).start()

    def exchange(phase, own, norm, weights, gate, mid, final):
        def ready(block, first=0, count=rows):
            source = own if block == SAME else held.at[phase, block]
            prepare(phase, source, block, first, count, norm, weights, gate)

        def join(*jobs):
            close(phase, [(block, 0, rows, group) for block, group in jobs], mid, final)

        def await_line(target, part):
            line_copy(phase, target, part, own).wait_recv()

        def relay(part):
            await_line(OVER, part)
            line_copy(phase, BOTH, part).start()

        def await_all(target):
            for part in range(pieces):
                await_line(target, part)

        def take_across():
            take_fixed(phase, ACROSS)
            fixed_copy(phase, ACROSS, PEER).start()

        def hand_on():
            landed_wait(phase, (SAME, SIDE))
            turn_strip(0)
            send_strip(0)

        ready(SAME)
        take_fixed(phase, PEER)
        join((SAME, NEAR))

        @pl.when(end)
        def _():
            take_across()
            await_all(SIDE)
            ready(SIDE)
            join((SAME, (ACROSS,)), (SIDE, NEAR + (ACROSS,)))
            relay(0)
            relay(1)
            take_fixed(phase, CORNER)
            join((SAME, (CORNER,)), (SIDE, (CORNER,)))
            relay(2)
            relay(3)
            relay(4)
            relay(5)
            ready(OVER)
            join((OVER, ALL))
            await_all(BOTH)
            ready(BOTH)
            join((BOTH, FAR))
            hand_on()
            join((BOTH, NEAR))

        @pl.when(jnp.logical_not(end))
        def _():
            fixed_copy(phase, OWN, ACROSS).wait_send()
            send_line(phase, own, OVER)
            for part in range(pieces):
                relay(part)
            ready(OVER)
            join((OVER, NEAR))
            await_all(SIDE)
            ready(SIDE)
            join((SIDE, NEAR))
            take_across()
            join((SAME, (ACROSS,)), (SIDE, (ACROSS,)))
            await_all(BOTH)
            ready(BOTH)
            take_fixed(phase, CORNER)
            join((SAME, (CORNER,)), (SIDE, (CORNER,)))
            join((OVER, FAR), (BOTH, FAR))
            hand_on()
            join((BOTH, NEAR))

    def landed_wait(phase, picked):
        for block in picked:
            for which in (PEER, ACROSS, CORNER):
                closed_wait(phase, block, which)

    def exchange_strips(norm, own_weights, weights, gate, mid, final):
        def ready(block, chunk):
            prepare_strip(block, chunk, norm, weights, gate)

        def join(*jobs):
            close(1, [(block, 0, rows, group) for block, group in jobs], mid, final)

        own_strip(0, norm, own_weights)
        ready(SAME, 0)
        landed_wait(0, (OVER, BOTH))
        turn_strip(1)
        send_strip(1)
        own_strip(1, norm, own_weights)
        ready(SAME, 1)
        for chunk in range(HALVES):
            take_fixed_strip(PEER, chunk)
        join((SAME, NEAR))
        for part in range(STRIP_PIECES):
            relay_strip(1, part)
        await_strip(SIDE, 0)
        ready(SIDE, 0)
        ready(OVER, 1)
        await_strip(SIDE, 1)
        ready(SIDE, 1)
        join((SIDE, NEAR))
        relay_strip(0, 0)
        for chunk in range(HALVES):
            take_fixed_strip(ACROSS, chunk)
            fixed_strip_copy(ACROSS, PEER, chunk).start()
        relay_strip(0, 1)
        join((SAME, (ACROSS,)), (SIDE, (ACROSS,)))
        relay_strip(0, 2)
        ready(OVER, 0)
        await_strip(BOTH, 1)
        ready(BOTH, 1)
        for chunk in range(HALVES):
            take_fixed_strip(CORNER, chunk)
        join((SAME, (CORNER,)), (SIDE, (CORNER,)), (OVER, ALL))
        await_strip(BOTH, 0)
        ready(BOTH, 0)
        join((BOTH, FAR))
        join((BOTH, NEAR))
        landed_wait(1, (SAME, SIDE, OVER, BOTH))

    def turn(phase, target):
        turned[...] = landed[phase].reshape(tokens * SUB, channels).astype(jnp.float32)
        for row in range(rows):
            target[row] = turned[pl.ds(row, tokens, stride=SUB), :].astype(jnp.bfloat16)

    def finish(phase, own):
        for part in range(pieces):
            for target in (SIDE, OVER, BOTH):
                line_copy(phase, target, part, own).wait_send()
        fixed_copy(phase, OWN, PEER).wait_send()

        @pl.when(end)
        def _():
            fixed_copy(phase, OWN, ACROSS).wait_send()

        fixed_copy(phase, ACROSS, PEER).wait_send()
        finish_closed(phase)

    def finish_closed(phase):
        for block in range(blocks):
            for which in (PEER, ACROSS, CORNER):
                closed_copy(phase, block, which, pl.ds(0, rows)).wait_send()

    def send_line(phase, own, target):
        for part in range(pieces):
            line_copy(phase, target, part, own).start()

    def early_over(phase, own):
        send_line(phase, own, SIDE)

        @pl.when(end)
        def _():
            send_line(phase, own, OVER)

    def launch(phase, own):
        fixed_copy(phase, OWN, ACROSS).start()
        fixed_copy(phase, OWN, PEER).start()

    def load(at):
        return pltpu.make_async_copy(inputs[at], copies[at], loaded.at[at])

    first_inputs = 3
    barrier = pltpu.get_barrier_semaphore()

    def greet(device):
        pl.semaphore_signal(barrier, inc=1, device_id={"axial": device}, device_id_type=MESH)

    for which in (PEER, ACROSS, CORNER):
        greet(mate(which))
    greet(device(SIDE, OWN))
    greet(device(OVER, OWN))
    for at in range(INPUTS):
        load(at).start()
    tri[...] = jnp.zeros_like(tri)
    normed_ref[...] = jnp.zeros_like(normed_ref)
    raw_ref[...] = jnp.zeros_like(raw_ref)
    split = 2 * hidden
    for at in range(first_inputs):
        load(at).wait()
    own_side(0, pair_ref[...], norm_out, proj_out[:, split:])
    pl.semaphore_wait(barrier, QUAD + 1)
    early_over(0, pair_ref)
    launch(0, pair_ref)
    for at in range(first_inputs, INPUTS):
        load(at).wait()
    exchange(0, pair_ref, norm_out, proj_out[:, :split], gate_out, mid_out, final_out)
    exchange_strips(norm_in, proj_in[:, :split], proj_in[:, split:], gate_in, mid_in, final_in)
    turn(1, out_ref)
    finish(0, pair_ref)
    for chunk in range(HALVES):
        for part in range(STRIP_PIECES):
            for target in (SIDE, OVER, BOTH):
                strip_copy(target, chunk, part).wait_send()
        fixed_strip_copy(OWN, PEER, chunk).wait_send()
        fixed_strip_copy(OWN, ACROSS, chunk).wait_send()
        fixed_strip_copy(ACROSS, PEER, chunk).wait_send()
    finish_closed(1)


def gather_rows(devices, pair_rep, *weights):
    rows, tokens, channels = pair_rep.shape
    hidden = weights[1].shape[1] // 4
    gains = [w.reshape(1, -1) if w.ndim == 1 else w for w in weights]
    blocks = devices // QUAD
    pieces = PIECES
    block = (rows, tokens, hidden)
    low, full = jnp.bfloat16, jnp.float32
    return pl.pallas_call(
        functools.partial(line_kernel, devices, pieces),
        out_shape=jax.ShapeDtypeStruct(pair_rep.shape, pair_rep.dtype),
        in_specs=[pl.BlockSpec(memory_space=pl.ANY)] * INPUTS,
        out_specs=pl.BlockSpec(memory_space=pltpu.VMEM),
        scratch_shapes=[pltpu.VMEM(array.shape, array.dtype) for array in (pair_rep, *gains)]
        + [
            pltpu.SemaphoreType.DMA((INPUTS,)),
            pltpu.VMEM((1, blocks) + block, low),
            pltpu.VMEM((1, QUAD) + block, low),
            pltpu.VMEM((blocks, HALVES, rows, tokens // HALVES, channels), low),
            pltpu.VMEM((QUAD, HALVES, rows, tokens // HALVES, hidden), low),
            pltpu.VMEM((QUAD,) + block, full),
            pltpu.VMEM((blocks,) + block, full),
            pltpu.VMEM((rows, tokens + SUB, channels), full),
            pltpu.VMEM((rows, tokens + SUB, channels), full),
            pltpu.VMEM((blocks, rows, QUAD, SUB, channels), full),
            pltpu.VMEM((blocks, rows, QUAD, SUB, channels), full),
            pltpu.VMEM((blocks, rows, QUAD, SUB, channels), full),
            pltpu.VMEM((2, blocks, QUAD, rows, SUB, channels), low),
            pltpu.VMEM((2, devices, rows, SUB, channels), low),
            pltpu.VMEM((tokens * SUB, channels), full),
            pltpu.SemaphoreType.DMA((2, blocks, pieces)),
            pltpu.SemaphoreType.DMA((2, blocks, pieces)),
            pltpu.SemaphoreType.DMA((2, QUAD)),
            pltpu.SemaphoreType.DMA((2, QUAD)),
            pltpu.SemaphoreType.DMA((2, blocks, QUAD)),
            pltpu.SemaphoreType.DMA((2, devices)),
            pltpu.SemaphoreType.DMA((blocks, HALVES, STRIP_PIECES)),
            pltpu.SemaphoreType.DMA((blocks, HALVES, STRIP_PIECES)),
            pltpu.SemaphoreType.DMA((QUAD, HALVES)),
            pltpu.SemaphoreType.DMA((QUAD, HALVES)),
        ],
        compiler_params=pltpu.CompilerParams(
            collective_id=0, has_side_effects=True, vmem_limit_bytes=VMEM_BYTES
        ),
        name="gather_rows",
    )(pair_rep, *gains)


def exchange_channels(
    pair_rep,
    norm_out,
    proj_out,
    gate_out,
    mid_out,
    final_out,
    norm_in,
    proj_in,
    gate_in,
    mid_in,
    final_in,
):
    first = update(pair_rep, norm_out, proj_out, gate_out, mid_out, final_out, True)
    return update(first, norm_in, proj_in, gate_in, mid_in, final_in, False)


def solution(mesh):
    devices = mesh.shape["axial"]

    def on_device(*arrays):
        if fits(devices, arrays[0].shape, arrays[2].shape):
            return gather_rows(devices, *arrays)
        return exchange_channels(*arrays)

    placed = (P(("groups", "axial"), None, None), P(), P(), P(), P(), P(), P(), P(), P(), P(), P())
    return jax.shard_map(
        on_device,
        mesh=mesh,
        in_specs=placed,
        out_specs=P(("groups", "axial"), None, None),
        check_vma=False,
    )
```

```python
import functools

import jax
import jax.numpy as jnp
from jax import lax
from jax.experimental import pallas as pl
from jax.experimental.pallas import tpu as pltpu
from jax.sharding import PartitionSpec as P

EPS = 1e-05


def normalize(values, gain, axis):
    average = jnp.mean(values, axis=axis, keepdims=True)
    spread = jnp.mean(jnp.square(values - average), axis=axis, keepdims=True)
    return (values - average) * lax.rsqrt(spread + EPS) * gain


def channel_product(left_side, right_side, outgoing):
    formula = "kil,kjl->kij" if outgoing else "kli,klj->kij"
    got_left, got_right = (
        lax.all_to_all(left_side, "axial", split_axis=0, concat_axis=1, tiled=True),
        lax.all_to_all(right_side, "axial", split_axis=0, concat_axis=1, tiled=True),
    )
    return jnp.einsum(formula, got_left, got_right, preferred_element_type=jnp.float32)


def update(pair_rep, norm_gain, weights, gate_weight, mid_gain, final_weight, outgoing):
    normed = normalize(pair_rep.astype(jnp.float32), norm_gain, -1).astype(jnp.bfloat16)
    projected = jnp.einsum("rnc,ck->krn", normed, weights, preferred_element_type=jnp.float32)
    hidden = weights.shape[1] // 4
    left_side = (jax.nn.sigmoid(projected[hidden : 2 * hidden]) * projected[:hidden]).astype(
        jnp.bfloat16
    )
    right_side = (
        jax.nn.sigmoid(projected[3 * hidden :]) * projected[2 * hidden : 3 * hidden]
    ).astype(jnp.bfloat16)
    product = channel_product(left_side, right_side, outgoing)
    tri = lax.all_to_all(
        product.astype(jnp.bfloat16), "axial", split_axis=1, concat_axis=0, tiled=True
    )
    gating = jax.nn.sigmoid(
        jnp.einsum("rnc,ce->rne", normed, gate_weight, preferred_element_type=jnp.float32)
    )
    tri_normed = normalize(tri.astype(jnp.float32), mid_gain[:, None, None], 0).astype(jnp.bfloat16)
    result = jnp.einsum("krn,kc->rnc", tri_normed, final_weight, preferred_element_type=jnp.float32)
    return (pair_rep.astype(jnp.float32) + gating * result).astype(jnp.bfloat16)


MESH = pl.DeviceIdType.MESH
CORES = 2
SIDES = 2
QUAD = CORES * 2
SAME, SIDE, OVER, BOTH = range(4)
OWN, PEER, ACROSS, CORNER = range(4)
NEAR, FAR, ALL = (OWN, PEER), (ACROSS, CORNER), (OWN, PEER, ACROSS, CORNER)
SUB = 8
HALVES = 2
PAIR = 2
INPUTS = 11
PIECES = 6
STRIP_PIECES = 3
VMEM_BYTES = 56 * 1024 * 1024


def fits(devices, pair_shape, proj_shape):
    rows, tokens, channels = pair_shape
    hidden = proj_shape[1] // 4
    block = rows * tokens * hidden * 4
    return (
        devices == QUAD * SIDES * HALVES
        and devices * rows == tokens
        and rows <= SUB
        and rows % PIECES == 0
        and rows % PAIR == 0
        and rows % STRIP_PIECES == 0
        and tokens % (16 * HALVES) == 0
        and rows > SUB // 2
        and tokens % 16 == 0
        and channels == hidden
        and hidden % 128 == 0
        and (6 * (devices // QUAD) + 24) * block < VMEM_BYTES // 2
    )


def layer_norm(values, gain):
    average = jnp.mean(values, axis=-1, keepdims=True)
    centred = values - average
    spread = jnp.mean(jnp.square(centred), axis=-1, keepdims=True)
    return centred * lax.rsqrt(spread + EPS) * gain


def dot(left, right):
    return jnp.dot(left, right, preferred_element_type=jnp.float32)


def line_kernel(
    devices,
    pieces,
    *refs,
):
    inputs, out_ref, scratch = refs[:INPUTS], refs[INPUTS], refs[INPUTS + 1 :]
    copies, scratch = scratch[:INPUTS], scratch[INPUTS:]
    (
        pair_ref,
        norm_out,
        proj_out,
        gate_out,
        mid_out,
        final_out,
        norm_in,
        proj_in,
        gate_in,
        mid_in,
        final_in,
    ) = copies
    (
    loaded,
    held,
    fixed,
    strips,
    fixed_strips,
    fixed_f32,
    moving,
    normed_ref,
    raw_ref,
    resid,
    gating,
    tri,
    closed,
    landed,
    turned,
    line_send,
    line_recv,
    fixed_send,
    fixed_recv,
    closed_send,
    closed_recv,
    strip_send,
    strip_recv,
    fixed_strip_send,
    fixed_strip_recv,
    ) = scratch
    rows, tokens, channels = pair_ref.shape
    hidden = fixed.shape[-1]
    blocks = devices // QUAD
    piece = rows // pieces
    me = lax.axis_index("axial")
    core = me % CORES
    side = (me // CORES) % SIDES
    level = me // (CORES * SIDES)
    half, floor = level // 2, level % 2
    end = jnp.logical_or(level == 0, level == 2 * HALVES - 1)
    places = ((0, 0), (0, 1), (1, 0), (1, 1))
    seats = ((0, 0), (0, 1), (1, 1), (1, 0))

    def turned_to(value, flip):
        return 1 - value if flip else value

    def device(block, which):
        over, aside = places[block]
        up, swap = seats[which]
        at = 2 * turned_to(half, over) + turned_to(floor, up)
        return (at * SIDES + turned_to(side, aside)) * CORES + turned_to(core, swap != aside)

    def mate(which):
        return device(SAME, which)

    def remote(source, target, sent, got, device):
        return pltpu.make_async_remote_copy(
            src_ref=source,
            dst_ref=target,
            send_sem=sent,
            recv_sem=got,
            device_id={"axial": device},
            device_id_type=MESH,
        )

    def window(part):
        return pl.ds(part * piece, piece)

    def line_copy(phase, target, part, source=None):
        came = held.at[phase, OVER, window(part)]
        goes = came if target == BOTH else source.at[window(part)]
        return remote(
            goes,
            held.at[phase, target, window(part)],
            line_send.at[phase, target, part],
            line_recv.at[phase, target, part],
            device(OVER if target == OVER else SIDE, OWN),
        )

    def fixed_copy(phase, which, to):
        arrives = {(OWN, PEER): PEER, (OWN, ACROSS): ACROSS, (ACROSS, PEER): CORNER}[which, to]
        return remote(
            fixed.at[phase, which],
            fixed.at[phase, arrives],
            fixed_send.at[phase, arrives],
            fixed_recv.at[phase, arrives],
            mate(to),
        )

    def closed_copy(phase, block, which, span):
        here = device(block, OWN)
        return remote(
            closed.at[phase, block, which, span, pl.ds(0, rows)],
            landed.at[phase, here, span, pl.ds(0, rows)],
            closed_send.at[phase, block, which],
            closed_recv.at[phase, here],
            mate(which),
        )

    def closed_wait(phase, block, which):
        there = device(block, which)
        remote(
            closed.at[phase, block, which, :, pl.ds(0, rows)],
            landed.at[phase, there, :, pl.ds(0, rows)],
            closed_send.at[phase, block, which],
            closed_recv.at[phase, there],
            mate(which),
        ).wait_recv()

    width = tokens // HALVES
    thick = rows // STRIP_PIECES

    def strip_copy(target, chunk, part):
        span = pl.ds(part * thick, thick)
        lands = 1 - chunk if target == OVER else chunk
        return remote(
            strips.at[OVER if target == BOTH else SAME, chunk, span],
            strips.at[target, lands, span],
            strip_send.at[target, chunk, part],
            strip_recv.at[target, lands, part],
            device(OVER if target == OVER else SIDE, OWN),
        )

    def strip_wait(target, chunk, part):
        strip_copy(target, 1 - chunk if target == OVER else chunk, part).wait_recv()

    def fixed_strip_copy(which, to, chunk):
        arrives = {(OWN, PEER): PEER, (OWN, ACROSS): ACROSS, (ACROSS, PEER): CORNER}[which, to]
        return remote(
            fixed_strips.at[which, chunk],
            fixed_strips.at[arrives, chunk],
            fixed_strip_send.at[arrives, chunk],
            fixed_strip_recv.at[arrives, chunk],
            mate(to),
        )

    def columns(chunk):
        return slice(chunk * width, (chunk + 1) * width)

    def send_strip(chunk):
        for part in range(STRIP_PIECES):
            strip_copy(OVER, chunk, part).start()
            strip_copy(SIDE, chunk, part).start()

    def relay_strip(chunk, part):
        strip_wait(OVER, chunk, part)
        strip_copy(BOTH, chunk, part).start()

    def await_strip(target, chunk):
        for part in range(STRIP_PIECES):
            strip_wait(target, chunk, part)

    def take_fixed_strip(which, chunk):
        source = ACROSS if which == CORNER else OWN
        fixed_strip_copy(source, ACROSS if which == ACROSS else PEER, chunk).wait_recv()
        fixed_f32[which, :, columns(chunk), :] = fixed_strips[which, chunk].astype(jnp.float32)

    def own_strip(chunk, norm, weights):
        values = flat(strips[SAME, chunk]).astype(jnp.float32)
        normed = layer_norm(values, norm[...]).astype(jnp.bfloat16)
        made = gated(dot(normed, weights)).reshape(rows, width, hidden)
        fixed_strips[OWN, chunk] = made
        fixed_f32[OWN, :, columns(chunk), :] = made.astype(jnp.float32)
        fixed_strip_copy(OWN, ACROSS, chunk).start()
        fixed_strip_copy(OWN, PEER, chunk).start()

    def turn_strip(chunk):
        group = devices // HALVES
        base = (half if chunk == 0 else 1 - half) * group
        size = group * rows * SUB
        picked = landed[0, pl.ds(base, group)].reshape(size, channels)
        turned[:size] = picked.astype(jnp.float32)
        for row in range(rows):
            taken = turned[pl.ds(row, width, stride=SUB), :]
            strips[SAME, chunk, row] = taken.astype(jnp.bfloat16)

    def flat(values):
        return values.reshape(-1, values.shape[-1])

    def gated(projected):
        return (jax.nn.sigmoid(projected[:, hidden:]) * projected[:, :hidden]).astype(jnp.bfloat16)

    def own_side(phase, block, norm, weights):
        normed = layer_norm(flat(block).astype(jnp.float32), norm[...]).astype(jnp.bfloat16)
        made = gated(dot(normed, weights)).reshape(rows, tokens, hidden)
        fixed[phase, OWN] = made
        fixed_f32[OWN] = made.astype(jnp.float32)

    def take_fixed(phase, which):
        source = ACROSS if which == CORNER else OWN
        fixed_copy(phase, source, ACROSS if which == ACROSS else PEER).wait_recv()
        fixed_f32[which] = fixed[phase, which].astype(jnp.float32)

    def prepare(phase, source, block, first, count, norm, weights, gate):
        span = pl.ds(first, count)
        raw = source[span].astype(jnp.float32)
        normed = layer_norm(flat(raw), norm[...])
        raw_ref[:count, :tokens] = raw
        normed_ref[:count, :tokens] = normed.reshape(count, tokens, channels)
        made = gated(dot(normed.astype(jnp.bfloat16), weights))
        moving[block, span] = made.astype(jnp.float32).reshape(count, tokens, hidden)
        picked = []
        for row in range(count):
            for which in range(QUAD):
                at = pl.ds(mate(which) * rows, SUB)
                picked.append(normed_ref[row, at, :])
                resid[block, first + row, which] = raw_ref[row, at, :]
        picked = jnp.concatenate(picked, axis=0).astype(jnp.bfloat16)
        opened = jax.nn.sigmoid(dot(picked, gate[...]))
        gating[block, span] = opened.reshape(count, QUAD, SUB, channels)

    def prepare_strip(block, chunk, norm, weights, gate):
        raw = strips[block, chunk].astype(jnp.float32)
        normed = layer_norm(flat(raw), norm[...])
        made = gated(dot(normed.astype(jnp.bfloat16), weights))
        made = made.astype(jnp.float32).reshape(rows, width, hidden)
        moving[block, :, columns(chunk), :] = made
        if chunk:
            return
        raw_ref[:, :width] = raw
        normed_ref[:, :width] = normed.reshape(rows, width, channels)
        picked = []
        for row in range(rows):
            for which in range(QUAD):
                at = pl.ds((mate(which) - half * (devices // HALVES)) * rows, SUB)
                picked.append(normed_ref[row, at, :])
                resid[block, row, which] = raw_ref[row, at, :]
        picked = jnp.concatenate(picked, axis=0).astype(jnp.bfloat16)
        opened = jax.nn.sigmoid(dot(picked, gate[...]))
        gating[block] = opened.reshape(rows, QUAD, SUB, channels)

    def fold(parts):
        place = lax.broadcasted_iota(jnp.int32, (SUB, hidden), 0)
        apart = SUB // 2
        while apart:
            first_half = (place // apart) % 2 == 0

            def joined(low, high):
                ahead = low + pltpu.roll(low, SUB - apart, 0)
                if high is None:
                    return jnp.where(first_half, ahead, low + pltpu.roll(low, apart, 0))
                return jnp.where(first_half, ahead, high + pltpu.roll(high, apart, 0))

            parts = parts + [None] * (2 * apart - len(parts))
            parts = [joined(parts[at], parts[at + apart]) for at in range(apart)]
            apart //= 2
        return parts[0]

    def tiles(values):
        return values.reshape(tokens // SUB, SUB, hidden)

    def multiply(jobs):
        def one(at, carry):
            for block, group in jobs:
                right = [tiles(moving[block, PAIR * at + row]) for row in range(PAIR)]
                for which in group:
                    sums = [[], []]
                    for own in range(rows):
                        left = tiles(fixed_f32[which, own])
                        for row in range(PAIR):
                            sums[row].append(jnp.sum(left * right[row], axis=0))
                    for row in range(PAIR):
                        tri[block, PAIR * at + row, which] = fold(sums[row])
            return carry

        lax.fori_loop(0, rows // PAIR, one, 0)

    def close(phase, jobs, mid, final):
        multiply([(block, group) for block, _, _, group in jobs])

        def gather(ref):
            picked = []
            for block, first, count, group in jobs:
                lanes = slice(group[0], group[-1] + 1)
                picked.append(flat(ref[block, first : first + count, lanes]))
            return jnp.concatenate(picked, axis=0) if len(picked) > 1 else picked[0]

        product = gather(tri).astype(jnp.bfloat16).astype(jnp.float32)
        normed = layer_norm(product, mid[...]).astype(jnp.bfloat16)
        result = gather(resid) + gather(gating) * dot(normed, final[...])
        result = result.astype(jnp.bfloat16)
        at = 0
        for block, first, count, group in jobs:
            size = count * len(group) * SUB
            part = result[at : at + size].reshape(count, len(group), SUB, channels)
            at += size
            span = pl.ds(first, count)
            for place, which in enumerate(group):
                if which == OWN:
                    landed[phase, device(block, OWN), span] = part[:, place]
                else:
                    closed[phase, block, which, span] = part[:, place]
        for block, first, count, group in jobs:
            for which in group:
                if which != OWN:
                    closed_copy(phase, block, which, pl.ds(first, count)).start()

    def exchange(phase, own, norm, weights, gate, mid, final):
        def ready(block, first=0, count=rows):
            source = own if block == SAME else held.at[phase, block]
            prepare(phase, source, block, first, count, norm, weights, gate)

        def join(*jobs):
            close(phase, [(block, 0, rows, group) for block, group in jobs], mid, final)

        def await_line(target, part):
            line_copy(phase, target, part, own).wait_recv()

        def relay(part):
            await_line(OVER, part)
            line_copy(phase, BOTH, part).start()

        def await_all(target):
            for part in range(pieces):
                await_line(target, part)

        def take_across():
            take_fixed(phase, ACROSS)
            fixed_copy(phase, ACROSS, PEER).start()

        def hand_on():
            landed_wait(phase, (SAME, SIDE))
            turn_strip(0)
            send_strip(0)

        ready(SAME)
        take_fixed(phase, PEER)
        join((SAME, NEAR))

        @pl.when(end)
        def _():
            take_across()
            await_all(SIDE)
            ready(SIDE)
            join((SAME, (ACROSS,)), (SIDE, NEAR + (ACROSS,)))
            relay(0)
            relay(1)
            take_fixed(phase, CORNER)
            join((SAME, (CORNER,)), (SIDE, (CORNER,)))
            relay(2)
            relay(3)
            relay(4)
            relay(5)
            ready(OVER)
            join((OVER, ALL))
            await_all(BOTH)
            ready(BOTH)
            join((BOTH, FAR))
            hand_on()
            join((BOTH, NEAR))

        @pl.when(jnp.logical_not(end))
        def _():
            fixed_copy(phase, OWN, ACROSS).wait_send()
            send_line(phase, own, OVER)
            for part in range(pieces):
                relay(part)
            ready(OVER)
            join((OVER, NEAR))
            await_all(SIDE)
            ready(SIDE)
            join((SIDE, NEAR))
            take_across()
            join((SAME, (ACROSS,)), (SIDE, (ACROSS,)))
            await_all(BOTH)
            ready(BOTH)
            take_fixed(phase, CORNER)
            join((SAME, (CORNER,)), (SIDE, (CORNER,)))
            join((OVER, FAR), (BOTH, FAR))
            hand_on()
            join((BOTH, NEAR))

    def landed_wait(phase, picked):
        for block in picked:
            for which in (PEER, ACROSS, CORNER):
                closed_wait(phase, block, which)

    def exchange_strips(norm, own_weights, weights, gate, mid, final):
        def ready(block, chunk):
            prepare_strip(block, chunk, norm, weights, gate)

        def join(*jobs):
            close(1, [(block, 0, rows, group) for block, group in jobs], mid, final)

        own_strip(0, norm, own_weights)
        ready(SAME, 0)
        landed_wait(0, (OVER, BOTH))
        turn_strip(1)
        send_strip(1)
        own_strip(1, norm, own_weights)
        ready(SAME, 1)
        for chunk in range(HALVES):
            take_fixed_strip(PEER, chunk)
        join((SAME, NEAR))
        for part in range(STRIP_PIECES):
            relay_strip(1, part)
        await_strip(SIDE, 0)
        ready(SIDE, 0)
        ready(OVER, 1)
        await_strip(SIDE, 1)
        ready(SIDE, 1)
        join((SIDE, NEAR))
        relay_strip(0, 0)
        for chunk in range(HALVES):
            take_fixed_strip(ACROSS, chunk)
            fixed_strip_copy(ACROSS, PEER, chunk).start()
        relay_strip(0, 1)
        join((SAME, (ACROSS,)), (SIDE, (ACROSS,)))
        relay_strip(0, 2)
        ready(OVER, 0)
        await_strip(BOTH, 1)
        ready(BOTH, 1)
        for chunk in range(HALVES):
            take_fixed_strip(CORNER, chunk)
        join((SAME, (CORNER,)), (SIDE, (CORNER,)), (OVER, ALL))
        await_strip(BOTH, 0)
        ready(BOTH, 0)
        join((BOTH, FAR))
        join((BOTH, NEAR))
        landed_wait(1, (SAME, SIDE, OVER, BOTH))

    def turn(phase, target):
        turned[: tokens * SUB] = landed[phase].reshape(tokens * SUB, channels).astype(jnp.float32)
        for row in range(rows):
            target[row] = turned[pl.ds(row, tokens, stride=SUB), :].astype(jnp.bfloat16)

    def finish(phase, own):
        for part in range(pieces):
            for target in (SIDE, OVER, BOTH):
                line_copy(phase, target, part, own).wait_send()
        fixed_copy(phase, OWN, PEER).wait_send()

        @pl.when(end)
        def _():
            fixed_copy(phase, OWN, ACROSS).wait_send()

        fixed_copy(phase, ACROSS, PEER).wait_send()
        finish_closed(phase)

    def finish_closed(phase):
        for block in range(blocks):
            for which in (PEER, ACROSS, CORNER):
                closed_copy(phase, block, which, pl.ds(0, rows)).wait_send()

    def send_line(phase, own, target):
        for part in range(pieces):
            line_copy(phase, target, part, own).start()

    def early_over(phase, own):
        send_line(phase, own, SIDE)

        @pl.when(end)
        def _():
            send_line(phase, own, OVER)

    def launch(phase, own):
        fixed_copy(phase, OWN, ACROSS).start()
        fixed_copy(phase, OWN, PEER).start()

    def load(at):
        return pltpu.make_async_copy(inputs[at], copies[at], loaded.at[at])

    first_inputs = 3
    barrier = pltpu.get_barrier_semaphore()

    def greet(device):
        pl.semaphore_signal(barrier, inc=1, device_id={"axial": device}, device_id_type=MESH)

    for which in (PEER, ACROSS, CORNER):
        greet(mate(which))
    greet(device(SIDE, OWN))
    greet(device(OVER, OWN))
    for at in range(INPUTS):
        load(at).start()
    tri[...] = jnp.zeros_like(tri)
    normed_ref[...] = jnp.zeros_like(normed_ref)
    raw_ref[...] = jnp.zeros_like(raw_ref)
    split = 2 * hidden
    for at in range(first_inputs):
        load(at).wait()
    own_side(0, pair_ref[...], norm_out, proj_out[:, split:])
    pl.semaphore_wait(barrier, QUAD + 1)
    early_over(0, pair_ref)
    launch(0, pair_ref)
    for at in range(first_inputs, INPUTS):
        load(at).wait()
    exchange(0, pair_ref, norm_out, proj_out[:, :split], gate_out, mid_out, final_out)
    exchange_strips(norm_in, proj_in[:, :split], proj_in[:, split:], gate_in, mid_in, final_in)
    turn(1, out_ref)
    finish(0, pair_ref)
    for chunk in range(HALVES):
        for part in range(STRIP_PIECES):
            for target in (SIDE, OVER, BOTH):
                strip_copy(target, chunk, part).wait_send()
        fixed_strip_copy(OWN, PEER, chunk).wait_send()
        fixed_strip_copy(OWN, ACROSS, chunk).wait_send()
        fixed_strip_copy(ACROSS, PEER, chunk).wait_send()
    finish_closed(1)


def gather_rows(devices, pair_rep, *weights):
    rows, tokens, channels = pair_rep.shape
    hidden = weights[1].shape[1] // 4
    gains = [w.reshape(1, -1) if w.ndim == 1 else w for w in weights]
    blocks = devices // QUAD
    pieces = PIECES
    block = (rows, tokens, hidden)
    low, full = jnp.bfloat16, jnp.float32
    return pl.pallas_call(
        functools.partial(line_kernel, devices, pieces),
        out_shape=jax.ShapeDtypeStruct(pair_rep.shape, pair_rep.dtype),
        in_specs=[pl.BlockSpec(memory_space=pl.ANY)] * INPUTS,
        out_specs=pl.BlockSpec(memory_space=pltpu.VMEM),
        scratch_shapes=[pltpu.VMEM(array.shape, array.dtype) for array in (pair_rep, *gains)]
        + [
            pltpu.SemaphoreType.DMA((INPUTS,)),
            pltpu.VMEM((1, blocks) + block, low),
            pltpu.VMEM((1, QUAD) + block, low),
            pltpu.VMEM((blocks, HALVES, rows, tokens // HALVES, channels), low),
            pltpu.VMEM((QUAD, HALVES, rows, tokens // HALVES, hidden), low),
            pltpu.VMEM((QUAD,) + block, full),
            pltpu.VMEM((blocks,) + block, full),
            pltpu.VMEM((rows, tokens + SUB, channels), full),
            pltpu.VMEM((rows, tokens + SUB, channels), full),
            pltpu.VMEM((blocks, rows, QUAD, SUB, channels), full),
            pltpu.VMEM((blocks, rows, QUAD, SUB, channels), full),
            pltpu.VMEM((blocks, rows, QUAD, SUB, channels), full),
            pltpu.VMEM((2, blocks, QUAD, rows, SUB, channels), low),
            pltpu.VMEM((2, devices, rows, SUB, channels), low),
            pltpu.VMEM(((tokens + SUB) * SUB, channels), full),
            pltpu.SemaphoreType.DMA((2, blocks, pieces)),
            pltpu.SemaphoreType.DMA((2, blocks, pieces)),
            pltpu.SemaphoreType.DMA((2, QUAD)),
            pltpu.SemaphoreType.DMA((2, QUAD)),
            pltpu.SemaphoreType.DMA((2, blocks, QUAD)),
            pltpu.SemaphoreType.DMA((2, devices)),
            pltpu.SemaphoreType.DMA((blocks, HALVES, STRIP_PIECES)),
            pltpu.SemaphoreType.DMA((blocks, HALVES, STRIP_PIECES)),
            pltpu.SemaphoreType.DMA((QUAD, HALVES)),
            pltpu.SemaphoreType.DMA((QUAD, HALVES)),
        ],
        compiler_params=pltpu.CompilerParams(
            collective_id=0, has_side_effects=True, vmem_limit_bytes=VMEM_BYTES
        ),
        name="gather_rows",
    )(pair_rep, *gains)


def exchange_channels(
    pair_rep,
    norm_out,
    proj_out,
    gate_out,
    mid_out,
    final_out,
    norm_in,
    proj_in,
    gate_in,
    mid_in,
    final_in,
):
    first = update(pair_rep, norm_out, proj_out, gate_out, mid_out, final_out, True)
    return update(first, norm_in, proj_in, gate_in, mid_in, final_in, False)


def solution(mesh):
    devices = mesh.shape["axial"]

    def on_device(*arrays):
        if fits(devices, arrays[0].shape, arrays[2].shape):
            return gather_rows(devices, *arrays)
        return exchange_channels(*arrays)

    placed = (P(("groups", "axial"), None, None), P(), P(), P(), P(), P(), P(), P(), P(), P(), P())
    return jax.shard_map(
        on_device,
        mesh=mesh,
        in_specs=placed,
        out_specs=P(("groups", "axial"), None, None),
        check_vma=False,
    )
```
